16 devices in a mesh: row: 4 (over z, y), col: 4 (over x, core).
Axes of the slice: x: 2, y: 2, z: 2, core: 2. Of those that a mesh axis runs over, the one named last changes fastest.
Arguments:
- v_mat: float32 [8192, 8192], P('row', 'col')
- t_fac: float32 [128, 64, 64], P('col')
- z_vec: float32 [8192, 1024], P(None, ('col', 'row'))
Outputs:
- output: float32 [8192, 1024], P('row', 'col')
All inputs are finite; a program needn't handle non-finite values.
Results may differ from the reference program's by a relative error of at most 0.001.
Values sent between devices are 32-bit elements.
A program may use at most 1 GiB of HBM per device.

```python
import jax
import jax.numpy as jnp
from jax import lax

MAT_ORDER = 8192
PANEL_WIDTH = 64
NUM_VECTORS = 1024
ROW_SHARDS = 4
COL_SHARDS = 4


def stored_to_global(mat_order, panel_width, shards):
    stored_idx = jnp.arange(mat_order, dtype=jnp.int32)
    per_shard = mat_order // shards
    shard_idx = stored_idx // per_shard
    within = stored_idx % per_shard
    block_idx = within // panel_width
    offset = within % panel_width
    return (block_idx * shards + shard_idx) * panel_width + offset


def build_factors(v_mat):
    panels = v_mat.reshape(MAT_ORDER, MAT_ORDER // PANEL_WIDTH, PANEL_WIDTH)
    gram_mat = jnp.einsum('nsb,nse->sbe', panels, panels)
    half_diag = 0.5 * jnp.diagonal(gram_mat, axis1=1, axis2=2)
    inv_factor = jnp.triu(gram_mat, 1) + half_diag[:, :, None] * jnp.eye(PANEL_WIDTH, dtype=jnp.float32)
    return jnp.triu(jnp.linalg.inv(inv_factor))


def setup_inputs(seed: int = 0) -> dict:
    rng_key = jax.random.key(seed)
    key_v, key_z = jax.random.split(rng_key)
    raw_vals = jax.random.normal(key_v, (MAT_ORDER, MAT_ORDER), jnp.float32)
    row_ids = stored_to_global(MAT_ORDER, PANEL_WIDTH, ROW_SHARDS)[:, None]
    col_ids = stored_to_global(MAT_ORDER, PANEL_WIDTH, COL_SHARDS)[None, :]
    unit_diag = (row_ids == col_ids).astype(jnp.float32)
    v_mat = jnp.where(row_ids > col_ids, raw_vals, unit_diag)
    t_fac = build_factors(v_mat)
    z_vec = jax.random.normal(key_z, (MAT_ORDER, NUM_VECTORS), jnp.float32)
    return {'v_mat': v_mat, 't_fac': t_fac, 'z_vec': z_vec}


def reference(v_mat, t_fac, z_vec):
    num_panels = MAT_ORDER // PANEL_WIDTH
    local_panels = num_panels // COL_SHARDS

    def apply_panel(x_cur, panel_idx):
        panel_slot = (panel_idx % COL_SHARDS) * local_panels + panel_idx // COL_SHARDS
        v_pan = lax.dynamic_slice_in_dim(v_mat, panel_slot * PANEL_WIDTH, PANEL_WIDTH, axis=1)
        t_pan = lax.dynamic_index_in_dim(t_fac, panel_slot, axis=0, keepdims=False)
        w_blk = jnp.dot(v_pan.T, x_cur, preferred_element_type=jnp.float32)
        y_blk = jnp.dot(t_pan, w_blk, preferred_element_type=jnp.float32)
        x_new = x_cur - jnp.dot(v_pan, y_blk, preferred_element_type=jnp.float32)
        return x_new, None

    x_out, _ = lax.scan(apply_panel, z_vec, jnp.arange(num_panels - 1, -1, -1))
    return x_out
```

```python
import jax
import jax.numpy as jnp
from jax import lax
from jax.experimental import pallas as pl
from jax.experimental.pallas import tpu as pltpu
from jax.sharding import PartitionSpec as P

F32 = jnp.float32
MESH = pl.DeviceIdType.MESH
TILE = 256
AHEAD = 8


def dot(a, b, ca, cb):
    return lax.dot_general(a, b, (((ca,), (cb,)), ((), ())), preferred_element_type=F32,
                           precision=lax.Precision.HIGHEST)


def make_kernel(rows, blocks):
    def tiles_of(h):
        return (blocks + 1 - h) // 2

    def tiles_before(h):
        k = blocks - 1 - h
        return ((k + 1) // 2) * ((k + 2) // 2)

    def body(v_hbm, t_hbm, z_hbm, x_ref, vbuf, vs, tall, zbuf, wacc, r1, ws, r2, y_ref, gacc, gr1, gs, gr2, tbuf, gab,
             vx_s, vsib_s, vfwd_s, vloc_s, v_r, tx_s, txc_s, tsib_s, tloc_s, t_r, z_s, zloc_s, z_r,
             p1_s, p1_r, p2_s, p2_r, g1_s, g1_r, g2_s, g2_r, d_s, d_r):
        r = lax.axis_index("row")
        c = lax.axis_index("col")
        core = c % 2
        cx, csib, cxc = (c + 2) % 4, c + 1 - 2 * core, 3 - c
        ry, rz, rd = r + 1 - 2 * (r % 2), (r + 2) % 4, 3 - r
        dev_x, dev_sib, dev_xc = (r, cx), (r, csib), (r, cxc)
        dev_y, dev_z, dev_d = (ry, c), (rz, c), (rd, c)

        def remote(src, dst, ss, rs, dev):
            return pltpu.make_async_remote_copy(src, dst, ss, rs, device_id=dev, device_id_type=MESH)

        barrier = pltpu.get_barrier_semaphore()
        for dev in (dev_x, dev_sib, dev_xc, dev_y, dev_z, dev_d):
            pl.semaphore_signal(barrier, 1, device_id=dev, device_id_type=MESH)
        pl.semaphore_wait(barrier, 6)

        def v_src(hh):
            n = TILE * tiles_of(hh)
            return v_hbm.at[pl.ds(rows - n, n), pl.ds(hh * 128, 128)]

        def v_dst(slot, hh):
            return vbuf.at[slot, pl.ds(TILE * tiles_before(hh), TILE * tiles_of(hh)), :]

        def v_x(hh):
            return remote(v_src(hh), v_dst(c, hh), vx_s.at[hh], v_r.at[c, hh], dev_x)

        def v_sib(hh):
            return remote(v_src(hh), v_dst(c, hh), vsib_s.at[hh], v_r.at[c, hh], dev_sib)

        def v_fwd(hh):
            return remote(v_dst(cx, hh), v_dst(cx, hh), vfwd_s.at[hh], v_r.at[cx, hh], dev_sib)

        def v_loc(hh):
            return pltpu.make_async_copy(v_src(hh), v_dst(c, hh), vloc_s.at[hh])

        def v_arrive(slot, hh):
            return remote(v_src(hh), v_dst(slot, hh), vx_s.at[hh], v_r.at[slot, hh], dev_x)

        def t_copies(h):
            return (remote(t_hbm.at[h, core], tall.at[c, h], tx_s.at[h], t_r.at[c, h], dev_x),
                    remote(t_hbm.at[h, 1 - core], tall.at[c, h], txc_s.at[h], t_r.at[c, h], dev_xc),
                    remote(t_hbm.at[h, 1 - core], tall.at[c, h], tsib_s.at[h], t_r.at[c, h], dev_sib))

        def t_loc(h):
            return pltpu.make_async_copy(t_hbm.at[h, core], tall.at[c, h], tloc_s.at[h])

        def t_arrive(slot, h):
            return remote(t_hbm.at[h, core], tall.at[slot, h], tx_s.at[h], t_r.at[slot, h], dev_x)

        def issue_v(hh):
            for cp in t_copies(hh):
                cp.start()
            t_loc(hh).start()
            v_x(hh).start()
            v_loc(hh).start()
            v_sib(hh).start()

        def collect_v(hh):
            v_arrive(cx, hh).wait_recv()
            v_fwd(hh).start()
            v_loc(hh).wait()
            v_arrive(csib, hh).wait_recv()
            v_arrive(cxc, hh).wait_recv()
            t_loc(hh).wait()
            for slot in (cx, csib, cxc):
                t_arrive(slot, hh).wait_recv()

        def z_copies(t):
            out = []
            for i, dev in enumerate((dev_y, dev_z, dev_d)):
                src = z_hbm.at[pl.ds(rows * dev[0] + TILE * t, TILE), :]
                out.append(remote(src, zbuf.at[r, pl.ds(TILE * t, TILE), :], z_s.at[i, t], z_r.at[r, t], dev))
            return out

        def z_loc(t):
            src = z_hbm.at[pl.ds(rows * r + TILE * t, TILE), :]
            return pltpu.make_async_copy(src, zbuf.at[r, pl.ds(TILE * t, TILE), :], zloc_s.at[t])

        def issue_z(t):
            for cp in z_copies(t):
                cp.start()
            z_loc(t).start()

        def collect_z(t):
            z_loc(t).wait()
            for src_r in (ry, rz, rd):
                dst = zbuf.at[src_r, pl.ds(TILE * t, TILE), :]
                remote(z_hbm.at[pl.ds(0, TILE), :], dst, z_s.at[0, t], z_r.at[src_r, t], dev_y).wait_recv()
            s = pl.ds(TILE * t, TILE)
            for i in range(4):
                x_ref[s, 64 * i:64 * i + 64] = zbuf[i, s, :]

        def steps(half):
            return (dev_y, dev_z) if half == 0 else (dev_z, dev_y)

        def w_p1(p, half):
            s = pl.ds(128 * half, 128)
            return remote(wacc.at[p, s], r1.at[p, s], p1_s.at[p, half], p1_r.at[p, half], steps(half)[0])

        def w_p2(p, half):
            s = pl.ds(128 * half, 128)
            return remote(ws.at[p, s], r2.at[p, s], p2_s.at[p, half], p2_r.at[p, half], steps(half)[1])

        def g_p1(half):
            s = pl.ds(224 * half, 224)
            return remote(gacc.at[s], gr1.at[s], g1_s.at[half], g1_r.at[half], steps(half)[0])

        def g_p2(half):
            s = pl.ds(224 * half, 224)
            return remote(gs.at[s], gr2.at[s], g2_s.at[half], g2_r.at[half], steps(half)[1])

        def over_tiles(n, fn):
            def pair(t, _):
                fn(2 * TILE * t, 2 * TILE)
                return 0
            lax.fori_loop(0, n // 2, pair, 0)

            @pl.when(n % 2 == 1)
            def _():
                fn(TILE * (n - 1), TILE)

        def regroup(h, slot):
            base = TILE * tiles_before(h)

            def one(t, _):
                s = pl.ds(pl.multiple_of(base + TILE * t, TILE), TILE)
                d = pl.ds(pl.multiple_of(TILE * t, TILE), TILE)
                for i in range(2):
                    a, b = vbuf[2 * i, s, :], vbuf[2 * i + 1, s, :]
                    low = lax.broadcasted_iota(jnp.int32, a.shape, 1) < 64
                    ar, br = pltpu.roll(a, 64, 1), pltpu.roll(b, 64, 1)
                    vs[slot, d, 128 * i:128 * i + 128] = jnp.where(low, a, br)
                    vs[slot, d, 256 + 128 * i:256 + 128 * i + 128] = jnp.where(low, ar, b)
                return 0
            lax.fori_loop(0, tiles_of(h), one, 0)

        def gram(h, slot):
            gacc[...] = jnp.zeros_like(gacc)
            y_ref[...] = jnp.zeros_like(y_ref)

            def one(off, n):
                s = pl.ds(pl.multiple_of(off, TILE), n)
                own = vs[slot, s, pl.ds(pl.multiple_of(256 * core, 256), 256)]
                y_ref[0:256, :] += dot(own, own, 0, 0)
                half = vs[slot, s, pl.ds(pl.multiple_of(256 + 128 * core, 128), 128)]
                gacc[0:256, :] += dot(vs[slot, s, 0:256], half, 0, 0)
            over_tiles(tiles_of(h), one)
            gacc[256:384, :] = y_ref[0:128, 128:256]
            gacc[384:448, 0:64] = y_ref[0:64, 64:128]
            gacc[384:448, 64:128] = y_ref[128:192, 192:256]

        def act_g():
            for half in range(2):
                g_p1(half).wait()
            gs[...] = gacc[...] + gr1[...]
            for half in range(2):
                g_p2(half).start()

        def share(slot):
            return (remote(tbuf.at[slot, core], tbuf.at[slot, core], d_s.at[slot, 0], d_r.at[slot, 0], dev_sib),
                    remote(gab.at[slot, core], gab.at[slot, core], d_s.at[slot, 1], d_r.at[slot, 1], dev_sib))

        def shared(slot):
            return (remote(tbuf.at[slot, 1 - core], tbuf.at[slot, 1 - core], d_s.at[slot, 0], d_r.at[slot, 0], dev_sib),
                    remote(gab.at[slot, 1 - core], gab.at[slot, 1 - core], d_s.at[slot, 1], d_r.at[slot, 1], dev_sib))

        def merge(h, slot):
            for half in range(2):
                g_p2(half).wait()
            g = gs[...] + gr2[...]
            gab[slot, core] = g[0:256]
            zero = jnp.zeros((64, 64), F32)

            def diag(a, b):
                return jnp.concatenate([jnp.concatenate([a, zero], 1), jnp.concatenate([zero, b], 1)], 0)
            t0, t1, t2, t3 = (tall[i, h] for i in range(4))
            low = g[384:448]
            off = dot(diag(low[:, 0:64], low[:, 64:128]), diag(t1, t3), 1, 0)
            off = -dot(diag(t0, t2), off, 1, 0)
            ta = jnp.concatenate([jnp.concatenate([t0, off[0:64, 0:64]], 1), jnp.concatenate([zero, t1], 1)], 0)
            tb = jnp.concatenate([jnp.concatenate([t2, off[64:128, 64:128]], 1), jnp.concatenate([zero, t3], 1)], 0)
            cross = -dot(ta, dot(g[256:384], tb, 1, 0), 1, 0)
            tbuf[slot, core, 0:128, 0:128] = ta
            tbuf[slot, core, 0:128, 128:256] = cross
            tbuf[slot, core, 128:256, 0:128] = jnp.zeros((128, 128), F32)
            tbuf[slot, core, 128:256, 128:256] = tb

        def product(h, slot, p):
            wacc[p] = jnp.zeros((256, 256), F32)
            row0 = rows - TILE * tiles_of(h)

            def one(off, n):
                s = pl.ds(pl.multiple_of(off, TILE), n)
                sx = pl.ds(pl.multiple_of(row0 + off, TILE), n)
                wacc[p] += dot(vs[slot, s, 256 * p:256 * p + 256], x_ref[sx, :], 0, 0)
            over_tiles(tiles_of(h), one)
            for half in range(2):
                w_p1(p, half).start()

        def act_w(p):
            for half in range(2):
                w_p1(p, half).wait()
            ws[p] = wacc[p] + r1[p]
            for half in range(2):
                w_p2(p, half).start()

        def reduced(p):
            for half in range(2):
                w_p2(p, half).wait()
            return ws[p] + r2[p]

        def update(h, slot):
            row0 = rows - TILE * tiles_of(h)

            def one(off, n):
                s = pl.ds(pl.multiple_of(off, TILE), n)
                sx = pl.ds(pl.multiple_of(row0 + off, TILE), n)
                x_ref[sx, :] -= dot(vs[slot, s, :], y_ref[...], 1, 0)
            over_tiles(tiles_of(h), one)

        last = blocks - 1
        for t in (rows // TILE - 1, rows // TILE - 2):
            issue_z(t)
        for hh in range(last, last - AHEAD, -1):
            issue_v(hh)
        collect_v(last)
        regroup(last, last % 2)
        gram(last, last % 2)
        for half in range(2):
            g_p1(half).start()
        act_g()
        merge(last, last % 2)
        for cp in share(last % 2):
            cp.start()

        def block_step(i, _):
            h = last - i
            slot = h % 2
            nslot = 1 - slot

            @pl.when(slot == 1)
            def _():
                collect_z((h - 1) // 2)

            @pl.when(jnp.logical_and(slot == 1, h >= 5))
            def _():
                issue_z((h - 1) // 2 - 2)

            product(h, slot, 1)
            product(h, slot, 0)
            for hh in range(blocks - AHEAD):
                @pl.when(h == hh + AHEAD)
                def _():
                    issue_v(hh)
            for hh in range(blocks - 1):
                @pl.when(h - 1 == hh)
                def _():
                    collect_v(hh)

            @pl.when(h > 0)
            def _():
                regroup(h - 1, nslot)
                gram(h - 1, nslot)
                for half in range(2):
                    g_p1(half).start()
            act_w(1)
            act_w(0)

            @pl.when(h > 0)
            def _():
                act_g()
            for cp in share(slot):
                cp.wait_send()
            for cp in shared(slot):
                cp.wait_recv()
            yb = dot(tbuf[slot, 1], reduced(1), 1, 0)
            y_ref[256:512, :] = yb
            wa = reduced(0) - dot(gab[slot, 0], yb[0:128], 1, 0) - dot(gab[slot, 1], yb[128:256], 1, 0)
            y_ref[0:256, :] = dot(tbuf[slot, 0], wa, 1, 0)

            @pl.when(h > 0)
            def _():
                merge(h - 1, nslot)
                for cp in share(nslot):
                    cp.start()
            update(h, slot)
            return 0

        lax.fori_loop(0, blocks, block_step, 0)
        for hh in range(blocks):
            v_x(hh).wait_send()
            v_sib(hh).wait_send()
            v_fwd(hh).wait_send()
            for cp in t_copies(hh):
                cp.wait_send()
        for t in range(rows // TILE):
            for cp in z_copies(t):
                cp.wait_send()

    return body


def solution(mesh):
    def local(v_loc, t_loc, z_loc):
        rows, cols = v_loc.shape
        blocks = cols // 128
        t_loc = t_loc.reshape(blocks, 2, 64, 64)
        tiles = ((blocks + 1) // 2) * ((blocks + 2) // 2)
        dma = pltpu.SemaphoreType.DMA
        hbm = pl.BlockSpec(memory_space=pl.ANY)
        return pl.pallas_call(
            make_kernel(rows, blocks),
            out_shape=jax.ShapeDtypeStruct((rows, 256), F32),
            in_specs=[hbm] * 3,
            out_specs=pl.BlockSpec(memory_space=pltpu.VMEM),
            scratch_shapes=[
                pltpu.VMEM((4, TILE * tiles, 128), F32),
                pltpu.VMEM((2, rows, 512), F32),
                pltpu.VMEM((4, blocks, 64, 64), F32),
                pltpu.VMEM((4, rows, 64), F32),
                pltpu.VMEM((2, 256, 256), F32), pltpu.VMEM((2, 256, 256), F32),
                pltpu.VMEM((2, 256, 256), F32), pltpu.VMEM((2, 256, 256), F32),
                pltpu.VMEM((512, 256), F32),
                pltpu.VMEM((448, 128), F32), pltpu.VMEM((448, 128), F32),
                pltpu.VMEM((448, 128), F32), pltpu.VMEM((448, 128), F32),
                pltpu.VMEM((2, 2, 256, 256), F32),
                pltpu.VMEM((2, 2, 256, 128), F32),
                dma((blocks,)), dma((blocks,)), dma((blocks,)), dma((blocks,)), dma((4, blocks)),
                dma((blocks,)), dma((blocks,)), dma((blocks,)), dma((blocks,)), dma((4, blocks)),
                dma((3, rows // TILE)), dma((rows // TILE,)), dma((4, rows // TILE)),
                dma((2, 2)), dma((2, 2)), dma((2, 2)), dma((2, 2)),
                dma((2,)), dma((2,)), dma((2,)), dma((2,)),
                dma((2, 2)), dma((2, 2)),
            ],
            compiler_params=pltpu.CompilerParams(collective_id=0, has_side_effects=True,
                                                 vmem_limit_bytes=67043328),
        )(v_loc, t_loc, z_loc)

    return jax.shard_map(local, mesh=mesh,
                         in_specs=(P('row', 'col'), P('col', None, None), P(None, ('col', 'row'))),
                         out_specs=P('row', 'col'), check_vma=False)
```

```python
import jax
import jax.numpy as jnp
from jax import lax
from jax.experimental import pallas as pl
from jax.experimental.pallas import tpu as pltpu
from jax.sharding import PartitionSpec as P

F32 = jnp.float32
MESH = pl.DeviceIdType.MESH
TILE = 256
AHEAD = 8
Z_AHEAD = 4


def dot(a, b, ca, cb):
    return lax.dot_general(a, b, (((ca,), (cb,)), ((), ())), preferred_element_type=F32,
                           precision=lax.Precision.HIGHEST)


def make_kernel(rows, blocks):
    def tiles_of(h):
        return (blocks + 1 - h) // 2

    def tiles_before(h):
        k = blocks - 1 - h
        return ((k + 1) // 2) * ((k + 2) // 2)

    def body(v_hbm, t_hbm, z_hbm, x_ref, vbuf, vs, tall, zbuf, wacc, r1, ws, r2, y_ref, gacc, gr1, gs, gr2, tbuf, gab,
             vx_s, vsib_s, vfwd_s, vloc_s, v_r, tx_s, txc_s, tsib_s, tloc_s, t_r, z_s, zloc_s, z_r,
             p1_s, p1_r, p2_s, p2_r, g1_s, g1_r, g2_s, g2_r, d_s, d_r):
        r = lax.axis_index("row")
        c = lax.axis_index("col")
        core = c % 2
        cx, csib, cxc = (c + 2) % 4, c + 1 - 2 * core, 3 - c
        ry, rz, rd = r + 1 - 2 * (r % 2), (r + 2) % 4, 3 - r
        dev_x, dev_sib, dev_xc = (r, cx), (r, csib), (r, cxc)
        dev_y, dev_z, dev_d = (ry, c), (rz, c), (rd, c)

        def remote(src, dst, ss, rs, dev):
            return pltpu.make_async_remote_copy(src, dst, ss, rs, device_id=dev, device_id_type=MESH)

        barrier = pltpu.get_barrier_semaphore()
        for dev in (dev_x, dev_sib, dev_xc, dev_y, dev_z, dev_d):
            pl.semaphore_signal(barrier, 1, device_id=dev, device_id_type=MESH)
        pl.semaphore_wait(barrier, 6)

        def v_src(hh):
            n = TILE * tiles_of(hh)
            return v_hbm.at[pl.ds(rows - n, n), pl.ds(hh * 128, 128)]

        def v_dst(slot, hh):
            return vbuf.at[slot, pl.ds(TILE * tiles_before(hh), TILE * tiles_of(hh)), :]

        def v_x(hh):
            return remote(v_src(hh), v_dst(c, hh), vx_s.at[hh], v_r.at[c, hh], dev_x)

        def v_sib(hh):
            return remote(v_src(hh), v_dst(c, hh), vsib_s.at[hh], v_r.at[c, hh], dev_sib)

        def v_fwd(hh):
            return remote(v_dst(cx, hh), v_dst(cx, hh), vfwd_s.at[hh], v_r.at[cx, hh], dev_sib)

        def v_loc(hh):
            return pltpu.make_async_copy(v_src(hh), v_dst(c, hh), vloc_s.at[hh])

        def v_arrive(slot, hh):
            return remote(v_src(hh), v_dst(slot, hh), vx_s.at[hh], v_r.at[slot, hh], dev_x)

        def t_copies(h):
            return (remote(t_hbm.at[h, core], tall.at[c, h], tx_s.at[h], t_r.at[c, h], dev_x),
                    remote(t_hbm.at[h, 1 - core], tall.at[c, h], txc_s.at[h], t_r.at[c, h], dev_xc),
                    remote(t_hbm.at[h, 1 - core], tall.at[c, h], tsib_s.at[h], t_r.at[c, h], dev_sib))

        def t_loc(h):
            return pltpu.make_async_copy(t_hbm.at[h, core], tall.at[c, h], tloc_s.at[h])

        def t_arrive(slot, h):
            return remote(t_hbm.at[h, core], tall.at[slot, h], tx_s.at[h], t_r.at[slot, h], dev_x)

        def issue_v(hh):
            for cp in t_copies(hh):
                cp.start()
            t_loc(hh).start()
            v_x(hh).start()
            v_loc(hh).start()
            v_sib(hh).start()

        def forward_v(hh):
            v_arrive(cx, hh).wait_recv()
            v_fwd(hh).start()

        def collect_v(hh):
            v_loc(hh).wait()
            v_arrive(csib, hh).wait_recv()
            v_arrive(cxc, hh).wait_recv()
            t_loc(hh).wait()
            for slot in (cx, csib, cxc):
                t_arrive(slot, hh).wait_recv()

        def z_src(to, t):
            return z_hbm.at[:, pl.ds(pl.multiple_of(rows * to + TILE * t, TILE), TILE)]

        def z_copies(t):
            out = []
            for i, dev in enumerate((dev_y, dev_z, dev_d)):
                out.append(remote(z_src(dev[0], t), zbuf.at[t, r], z_s.at[i, t], z_r.at[r, t], dev))
            return out

        def z_loc(t):
            return pltpu.make_async_copy(z_src(r, t), zbuf.at[t, r], zloc_s.at[t])

        def issue_z(t):
            for cp in z_copies(t):
                cp.start()
            z_loc(t).start()

        def collect_z(t):
            z_loc(t).wait()
            for src_r in (ry, rz, rd):
                remote(z_src(r, t), zbuf.at[t, src_r], z_s.at[0, t], z_r.at[src_r, t], dev_y).wait_recv()
            x_ref[pl.ds(pl.multiple_of(TILE * t, TILE), TILE), :] = zbuf[t].reshape(256, TILE).T

        def steps(half):
            return (dev_y, dev_z) if half == 0 else (dev_z, dev_y)

        def w_p1(p, half):
            s = pl.ds(128 * half, 128)
            return remote(wacc.at[p, s], r1.at[p, s], p1_s.at[p, half], p1_r.at[p, half], steps(half)[0])

        def w_p2(p, half):
            s = pl.ds(128 * half, 128)
            return remote(ws.at[p, s], r2.at[p, s], p2_s.at[p, half], p2_r.at[p, half], steps(half)[1])

        def g_p1(half):
            s = pl.ds(224 * half, 224)
            return remote(gacc.at[s], gr1.at[s], g1_s.at[half], g1_r.at[half], steps(half)[0])

        def g_p2(half):
            s = pl.ds(224 * half, 224)
            return remote(gs.at[s], gr2.at[s], g2_s.at[half], g2_r.at[half], steps(half)[1])

        def over_tiles(n, fn):
            def pair(t, _):
                fn(2 * TILE * t, 2 * TILE)
                return 0
            lax.fori_loop(0, n // 2, pair, 0)

            @pl.when(n % 2 == 1)
            def _():
                fn(TILE * (n - 1), TILE)

        def regroup(h, slot):
            base = TILE * tiles_before(h)

            def one(t, _):
                s = pl.ds(pl.multiple_of(base + TILE * t, TILE), TILE)
                d = pl.ds(pl.multiple_of(TILE * t, TILE), TILE)
                for i in range(2):
                    a, b = vbuf[2 * i, s, :], vbuf[2 * i + 1, s, :]
                    low = lax.broadcasted_iota(jnp.int32, a.shape, 1) < 64
                    ar, br = pltpu.roll(a, 64, 1), pltpu.roll(b, 64, 1)
                    vs[slot, d, 128 * i:128 * i + 128] = jnp.where(low, a, br)
                    vs[slot, d, 256 + 128 * i:256 + 128 * i + 128] = jnp.where(low, ar, b)
                return 0
            lax.fori_loop(0, tiles_of(h), one, 0)

        def gram(h, slot):
            gacc[...] = jnp.zeros_like(gacc)
            y_ref[...] = jnp.zeros_like(y_ref)

            def one(off, n):
                s = pl.ds(pl.multiple_of(off, TILE), n)
                own = vs[slot, s, pl.ds(pl.multiple_of(256 * core, 256), 256)]
                y_ref[0:256, :] += dot(own, own, 0, 0)
                half = vs[slot, s, pl.ds(pl.multiple_of(256 + 128 * core, 128), 128)]
                gacc[0:256, :] += dot(vs[slot, s, 0:256], half, 0, 0)
            over_tiles(tiles_of(h), one)
            gacc[256:384, :] = y_ref[0:128, 128:256]
            gacc[384:448, 0:64] = y_ref[0:64, 64:128]
            gacc[384:448, 64:128] = y_ref[128:192, 192:256]

        def act_g():
            for half in range(2):
                g_p1(half).wait()
            gs[...] = gacc[...] + gr1[...]
            for half in range(2):
                g_p2(half).start()

        def share(slot):
            return (remote(tbuf.at[slot, core], tbuf.at[slot, core], d_s.at[slot, 0], d_r.at[slot, 0], dev_sib),
                    remote(gab.at[slot, core], gab.at[slot, core], d_s.at[slot, 1], d_r.at[slot, 1], dev_sib))

        def shared(slot):
            return (remote(tbuf.at[slot, 1 - core], tbuf.at[slot, 1 - core], d_s.at[slot, 0], d_r.at[slot, 0], dev_sib),
                    remote(gab.at[slot, 1 - core], gab.at[slot, 1 - core], d_s.at[slot, 1], d_r.at[slot, 1], dev_sib))

        def merge(h, slot):
            for half in range(2):
                g_p2(half).wait()
            g = gs[...] + gr2[...]
            gab[slot, core] = g[0:256]
            zero = jnp.zeros((64, 64), F32)

            def diag(a, b):
                return jnp.concatenate([jnp.concatenate([a, zero], 1), jnp.concatenate([zero, b], 1)], 0)
            t0, t1, t2, t3 = (tall[i, h] for i in range(4))
            low = g[384:448]
            off = dot(diag(low[:, 0:64], low[:, 64:128]), diag(t1, t3), 1, 0)
            off = -dot(diag(t0, t2), off, 1, 0)
            ta = jnp.concatenate([jnp.concatenate([t0, off[0:64, 0:64]], 1), jnp.concatenate([zero, t1], 1)], 0)
            tb = jnp.concatenate([jnp.concatenate([t2, off[64:128, 64:128]], 1), jnp.concatenate([zero, t3], 1)], 0)
            cross = -dot(ta, dot(g[256:384], tb, 1, 0), 1, 0)
            tbuf[slot, core, 0:128, 0:128] = ta
            tbuf[slot, core, 0:128, 128:256] = cross
            tbuf[slot, core, 128:256, 0:128] = jnp.zeros((128, 128), F32)
            tbuf[slot, core, 128:256, 128:256] = tb

        def product(h, slot, p):
            wacc[p] = jnp.zeros((256, 256), F32)
            row0 = rows - TILE * tiles_of(h)

            def one(off, n):
                s = pl.ds(pl.multiple_of(off, TILE), n)
                sx = pl.ds(pl.multiple_of(row0 + off, TILE), n)
                wacc[p] += dot(vs[slot, s, 256 * p:256 * p + 256], x_ref[sx, :], 0, 0)
            over_tiles(tiles_of(h), one)
            for half in range(2):
                w_p1(p, half).start()

        def act_w(p):
            for half in range(2):
                w_p1(p, half).wait()
            ws[p] = wacc[p] + r1[p]
            for half in range(2):
                w_p2(p, half).start()

        def reduced(p):
            for half in range(2):
                w_p2(p, half).wait()
            return ws[p] + r2[p]

        def update(h, slot):
            row0 = rows - TILE * tiles_of(h)

            def one(off, n):
                s = pl.ds(pl.multiple_of(off, TILE), n)
                sx = pl.ds(pl.multiple_of(row0 + off, TILE), n)
                x_ref[sx, :] -= dot(vs[slot, s, :], y_ref[...], 1, 0)
            over_tiles(tiles_of(h), one)

        last = blocks - 1
        top = rows // TILE - 1
        issue_v(last)
        issue_z(top)
        for hh in range(last - 1, last - AHEAD, -1):
            issue_v(hh)
        for t in range(top - 1, top - Z_AHEAD, -1):
            issue_z(t)
        forward_v(last)
        forward_v(last - 1)
        collect_v(last)
        regroup(last, last % 2)
        gram(last, last % 2)
        for half in range(2):
            g_p1(half).start()
        act_g()

        def block_step(i, _):
            h = last - i
            slot = h % 2
            nslot = 1 - slot

            @pl.when(slot == 1)
            def _():
                collect_z((h - 1) // 2)

            product(h, slot, 1)
            product(h, slot, 0)
            merge(h, slot)
            for cp in share(slot):
                cp.start()
            act_w(1)
            for hh in range(blocks - 2):
                @pl.when(h - 2 == hh)
                def _():
                    forward_v(hh)
            for hh in range(blocks - AHEAD):
                @pl.when(h == hh + AHEAD)
                def _():
                    issue_v(hh)
            for hh in range(blocks - 1):
                @pl.when(h - 1 == hh)
                def _():
                    collect_v(hh)

            @pl.when(h > 0)
            def _():
                regroup(h - 1, nslot)
            act_w(0)

            @pl.when(h > 0)
            def _():
                gram(h - 1, nslot)
                for half in range(2):
                    g_p1(half).start()
            for cp in share(slot):
                cp.wait_send()
            for cp in shared(slot):
                cp.wait_recv()
            yb = dot(tbuf[slot, 1], reduced(1), 1, 0)
            y_ref[256:512, :] = yb
            wa = reduced(0) - dot(gab[slot, 0], yb[0:128], 1, 0) - dot(gab[slot, 1], yb[128:256], 1, 0)
            y_ref[0:256, :] = dot(tbuf[slot, 0], wa, 1, 0)

            @pl.when(jnp.logical_and(slot == 1, h >= 2 * Z_AHEAD + 1))
            def _():
                issue_z((h - 1) // 2 - Z_AHEAD)
            update(h, slot)

            @pl.when(h > 0)
            def _():
                act_g()
            return 0

        lax.fori_loop(0, blocks, block_step, 0)
        for hh in range(blocks):
            v_x(hh).wait_send()
            v_sib(hh).wait_send()
            v_fwd(hh).wait_send()
            for cp in t_copies(hh):
                cp.wait_send()
        for t in range(rows // TILE):
            for cp in z_copies(t):
                cp.wait_send()

    return body


def solution(mesh):
    def local(v_loc, t_loc, z_loc):
        rows, cols = v_loc.shape
        blocks = cols // 128
        t_loc = t_loc.reshape(blocks, 2, 64, 64)
        tiles = ((blocks + 1) // 2) * ((blocks + 2) // 2)
        dma = pltpu.SemaphoreType.DMA
        hbm = pl.BlockSpec(memory_space=pl.ANY)
        return pl.pallas_call(
            make_kernel(rows, blocks),
            out_shape=jax.ShapeDtypeStruct((rows, 256), F32),
            in_specs=[hbm] * 3,
            out_specs=pl.BlockSpec(memory_space=pltpu.VMEM),
            scratch_shapes=[
                pltpu.VMEM((4, TILE * tiles, 128), F32),
                pltpu.VMEM((2, rows, 512), F32),
                pltpu.VMEM((4, blocks, 64, 64), F32),
                pltpu.VMEM((rows // TILE, 4, 64, TILE), F32),
                pltpu.VMEM((2, 256, 256), F32), pltpu.VMEM((2, 256, 256), F32),
                pltpu.VMEM((2, 256, 256), F32), pltpu.VMEM((2, 256, 256), F32),
                pltpu.VMEM((512, 256), F32),
                pltpu.VMEM((448, 128), F32), pltpu.VMEM((448, 128), F32),
                pltpu.VMEM((448, 128), F32), pltpu.VMEM((448, 128), F32),
                pltpu.VMEM((2, 2, 256, 256), F32),
                pltpu.VMEM((2, 2, 256, 128), F32),
                dma((blocks,)), dma((blocks,)), dma((blocks,)), dma((blocks,)), dma((4, blocks)),
                dma((blocks,)), dma((blocks,)), dma((blocks,)), dma((blocks,)), dma((4, blocks)),
                dma((3, rows // TILE)), dma((rows // TILE,)), dma((4, rows // TILE)),
                dma((2, 2)), dma((2, 2)), dma((2, 2)), dma((2, 2)),
                dma((2,)), dma((2,)), dma((2,)), dma((2,)),
                dma((2, 2)), dma((2, 2)),
            ],
            compiler_params=pltpu.CompilerParams(collective_id=0, has_side_effects=True,
                                                 vmem_limit_bytes=67043328),
        )(v_loc, t_loc, z_loc.T)

    return jax.shard_map(local, mesh=mesh,
                         in_specs=(P('row', 'col'), P('col', None, None), P(None, ('col', 'row'))),
                         out_specs=P('row', 'col'), check_vma=False)
```

```python
import jax
import jax.numpy as jnp
from jax import lax
from jax.experimental import pallas as pl
from jax.experimental.pallas import tpu as pltpu
from jax.sharding import PartitionSpec as P

F32 = jnp.float32
BF16 = jnp.bfloat16
MESH = pl.DeviceIdType.MESH
TILE = 256
AHEAD = 8
Z_START = 4
SWITCH = 10


def dot(a, b, ca, cb):
    return lax.dot_general(a, b, (((ca,), (cb,)), ((), ())), preferred_element_type=F32,
                           precision=lax.Precision.HIGHEST)


def split(a):
    a1 = a.astype(BF16)
    rest = a - a1.astype(F32)
    a2 = rest.astype(BF16)
    return a1, a2, (rest - a2.astype(F32)).astype(BF16)


def dot6(pairs, ca, cb):
    lhs, rhs = [], []
    for (a1, a2, a3), (b1, b2, b3) in pairs:
        lhs += [a3, a1, a2, a1, a2, a1]
        rhs += [b1, b3, b2, b2, b1, b1]
    return lax.dot_general(jnp.concatenate(lhs, ca), jnp.concatenate(rhs, cb), (((ca,), (cb,)), ((), ())),
                           preferred_element_type=F32)


def make_kernel(rows, blocks):
    def tiles_of(h):
        return (blocks + 1 - h) // 2

    def tiles_before(h):
        k = blocks - 1 - h
        return ((k + 1) // 2) * ((k + 2) // 2)

    area = TILE * tiles_before(-1)

    def body(v_hbm, t_hbm, z_hbm, o_ref, vbuf, vp, tall, xt, wacc, r1, ws, r2, yp, gkk, gacc, gr1, gs, gr2, tbuf, gab,
             nbuf, vx_s, vsib_s, vfwd_s, vloc_s, v_r, tx_s, txc_s, tsib_s, tloc_s, t_r, z_s, zloc_s, z_r,
             p1_s, p1_r, p2_s, p2_r, g1_s, g1_r, g2_s, g2_r, d_s, d_r):
        r = lax.axis_index("row")
        c = lax.axis_index("col")
        core = c % 2
        cx, csib, cxc = (c + 2) % 4, c + 1 - 2 * core, 3 - c
        ry, rz, rd = r + 1 - 2 * (r % 2), (r + 2) % 4, 3 - r
        dev_x, dev_sib, dev_xc = (r, cx), (r, csib), (r, cxc)
        dev_y, dev_z, dev_d = (ry, c), (rz, c), (rd, c)

        def remote(src, dst, ss, rs, dev):
            return pltpu.make_async_remote_copy(src, dst, ss, rs, device_id=dev, device_id_type=MESH)

        barrier = pltpu.get_barrier_semaphore()
        for dev in (dev_x, dev_sib, dev_xc, dev_y, dev_z, dev_d):
            pl.semaphore_signal(barrier, 1, device_id=dev, device_id_type=MESH)
        pl.semaphore_wait(barrier, 6)

        def v_src(hh):
            n = TILE * tiles_of(hh)
            return v_hbm.at[pl.ds(rows - n, n), pl.ds(hh * 128, 128)]

        def v_dst(rel, hh):
            return vbuf.at[pl.ds(area * (rel - 1) + TILE * tiles_before(hh), TILE * tiles_of(hh)), :]

        def v_x(hh):
            return remote(v_src(hh), v_dst(2, hh), vx_s.at[hh], v_r.at[1, hh], dev_x)

        def v_sib(hh):
            return remote(v_src(hh), v_dst(1, hh), vsib_s.at[hh], v_r.at[0, hh], dev_sib)

        def v_fwd(hh):
            return remote(v_dst(2, hh), v_dst(3, hh), vfwd_s.at[hh], v_r.at[2, hh], dev_sib)

        def v_loc(hh):
            dst = vbuf.at[pl.ds(3 * area + rows * (hh % 2), TILE * tiles_of(hh)), :]
            return pltpu.make_async_copy(v_src(hh), dst, vloc_s.at[hh])

        def v_arrive(rel, hh):
            return remote(v_src(hh), v_dst(rel, hh), vx_s.at[hh], v_r.at[rel - 1, hh], dev_x)

        def t_copies(h):
            return (remote(t_hbm.at[h, core], tall.at[c, h], tx_s.at[h], t_r.at[c, h], dev_x),
                    remote(t_hbm.at[h, 1 - core], tall.at[c, h], txc_s.at[h], t_r.at[c, h], dev_xc),
                    remote(t_hbm.at[h, 1 - core], tall.at[c, h], tsib_s.at[h], t_r.at[c, h], dev_sib))

        def t_loc(h):
            return pltpu.make_async_copy(t_hbm.at[h, core], tall.at[c, h], tloc_s.at[h])

        def t_arrive(slot, h):
            return remote(t_hbm.at[h, core], tall.at[slot, h], tx_s.at[h], t_r.at[slot, h], dev_x)

        def issue_v(hh):
            for cp in t_copies(hh):
                cp.start()
            t_loc(hh).start()
            v_x(hh).start()
            v_sib(hh).start()

        def forward_v(hh):
            v_arrive(2, hh).wait_recv()
            v_fwd(hh).start()

        def collect_v(hh):
            v_loc(hh).wait()
            v_arrive(1, hh).wait_recv()
            v_arrive(3, hh).wait_recv()
            t_loc(hh).wait()
            for slot in (cx, csib, cxc):
                t_arrive(slot, hh).wait_recv()

        def z_src(to, t):
            return z_hbm.at[:, pl.ds(pl.multiple_of(rows * to + TILE * t, TILE), TILE)]

        def z_dst(src_r, t):
            return xt.at[t, pl.ds(pl.multiple_of(64 * src_r, 64), 64), :]

        def z_copies(t):
            return [remote(z_src(dev[0], t), z_dst(r, t), z_s.at[i, t], z_r.at[r, t], dev)
                    for i, dev in enumerate((dev_y, dev_z, dev_d))]

        def z_loc(t):
            return pltpu.make_async_copy(z_src(r, t), z_dst(r, t), zloc_s.at[t])

        def issue_z(t):
            for cp in z_copies(t):
                cp.start()
            z_loc(t).start()

        def collect_z(t):
            z_loc(t).wait()
            for src_r in (ry, rz, rd):
                remote(z_src(r, t), z_dst(src_r, t), z_s.at[0, t], z_r.at[src_r, t], dev_y).wait_recv()

        def steps(half):
            return (dev_y, dev_z) if half == 0 else (dev_z, dev_y)

        def w_p1(p, half):
            s = pl.ds(128 * half, 128)
            return remote(wacc.at[p, s], r1.at[p, s], p1_s.at[p, half], p1_r.at[p, half], steps(half)[0])

        def w_p2(p, half):
            s = pl.ds(128 * half, 128)
            return remote(ws.at[p, s], r2.at[p, s], p2_s.at[p, half], p2_r.at[p, half], steps(half)[1])

        def g_p1(half):
            s = pl.ds(224 * half, 224)
            return remote(gacc.at[s], gr1.at[s], g1_s.at[half], g1_r.at[half], steps(half)[0])

        def g_p2(half):
            s = pl.ds(224 * half, 224)
            return remote(gs.at[s], gr2.at[s], g2_s.at[half], g2_r.at[half], steps(half)[1])

        def over_tiles(n, fn):
            def four(t, _):
                fn(4 * t, 4)
                return 0
            lax.fori_loop(0, n // 4, four, 0)

            @pl.when(n % 4 >= 2)
            def _():
                fn(4 * (n // 4), 2)

            @pl.when(n % 2 == 1)
            def _():
                fn(n - 1, 1)

        def prepare(h, slot):
            bases = []
            for i in range(4):
                rel = ((c // 2 + i // 2) % 2) * 2 + (c + i) % 2
                own = (3 - rel) // 3
                bases.append(own * (3 * area + rows * (h % 2)) + (1 - own) * (area * (rel - 1) + TILE * tiles_before(h)))

            def one(t, _):
                d = pl.ds(pl.multiple_of(TILE * t, TILE), TILE)
                for i in range(2):
                    a = vbuf[pl.ds(pl.multiple_of(bases[2 * i] + TILE * t, TILE), TILE), :]
                    b = vbuf[pl.ds(pl.multiple_of(bases[2 * i + 1] + TILE * t, TILE), TILE), :]
                    low = lax.broadcasted_iota(jnp.int32, a.shape, 1) < 64
                    ar, br = pltpu.roll(a, 64, 1), pltpu.roll(b, 64, 1)
                    for k, part in enumerate(split(jnp.where(low, a, br))):
                        vp[slot, k, d, 128 * i:128 * i + 128] = part
                    for k, part in enumerate(split(jnp.where(low, ar, b))):
                        vp[slot, k, d, 256 + 128 * i:256 + 128 * i + 128] = part
                return 0
            lax.fori_loop(0, tiles_of(h), one, 0)

        def parts(slot, t, lanes):
            s = pl.ds(pl.multiple_of(TILE * t, TILE), TILE)
            return tuple(vp[slot, k, s, lanes] for k in range(3))

        def gram(h, slot):
            gkk[...] = jnp.zeros_like(gkk)
            mine = pl.ds(pl.multiple_of(256 * core, 256), 256)
            half = pl.ds(pl.multiple_of(128 * core, 128), 128)

            def one(t, n):
                own = [parts(slot, t + u, mine) for u in range(n)]
                gkk[0:256, :] += dot6([(a, a) for a in own], 0, 0)
                gkk[256:384, :] += dot6([(parts(slot, t + u, half), parts(slot, t + u, pl.ds(256, 256)))
                                         for u in range(n)], 0, 0)
            over_tiles(tiles_of(h), one)
            gacc[0:128, :] = gkk[256:384, 0:128]
            gacc[128:256, :] = gkk[256:384, 128:256]
            gacc[256:384, :] = gkk[0:128, 128:256]
            gacc[384:448, 0:64] = gkk[0:64, 64:128]
            gacc[384:448, 64:128] = gkk[128:192, 192:256]

        def act_g():
            for half in range(2):
                g_p1(half).wait()
            gs[...] = gacc[...] + gr1[...]
            for half in range(2):
                g_p2(half).start()

        def rows_of(k):
            return pl.ds(pl.multiple_of(128 * k, 128), 128)

        def share(slot, k):
            return (remote(tbuf.at[slot, k], tbuf.at[slot, k], d_s.at[slot, 0], d_r.at[slot, 0], dev_sib),
                    remote(gab.at[slot, rows_of(k)], gab.at[slot, rows_of(k)], d_s.at[slot, 1], d_r.at[slot, 1], dev_sib))

        def merge(h, slot):
            for half in range(2):
                g_p2(half).wait()
            g = gs[...] + gr2[...]
            gab[slot, rows_of(core), 0:128] = g[0:128]
            gab[slot, rows_of(core), 128:256] = g[128:256]
            zero = jnp.zeros((64, 64), F32)

            def diag(a, b):
                return jnp.concatenate([jnp.concatenate([a, zero], 1), jnp.concatenate([zero, b], 1)], 0)
            t0, t1, t2, t3 = (tall[i, h] for i in range(4))
            low = g[384:448]
            off = dot(diag(low[:, 0:64], low[:, 64:128]), diag(t1, t3), 1, 0)
            off = -dot(diag(t0, t2), off, 1, 0)
            ta = jnp.concatenate([jnp.concatenate([t0, off[0:64, 0:64]], 1), jnp.concatenate([zero, t1], 1)], 0)
            tb = jnp.concatenate([jnp.concatenate([t2, off[64:128, 64:128]], 1), jnp.concatenate([zero, t3], 1)], 0)
            cross = -dot(ta, dot(g[256:384], tb, 1, 0), 1, 0)
            tbuf[slot, core, 0:128, 0:128] = ta
            tbuf[slot, core, 0:128, 128:256] = cross
            tbuf[slot, core, 128:256, 0:128] = jnp.zeros((128, 128), F32)
            tbuf[slot, core, 128:256, 128:256] = tb
            for cp in share(slot, core):
                cp.start()

        def factor(slot):
            for cp in share(slot, core):
                cp.wait_send()
            for cp in share(slot, 1 - core):
                cp.wait_recv()
            nbuf[...] = dot(tbuf[slot, 0], gab[slot], 1, 0)

        def product(h, slot, p):
            wacc[p] = jnp.zeros((256, 256), F32)
            t0 = rows // TILE - tiles_of(h)

            def one(t, n):
                wacc[p] += dot6([(split(xt[t0 + t + u]), parts(slot, t + u, pl.ds(256 * p, 256)))
                                 for u in range(n)], 1, 0)
            over_tiles(tiles_of(h), one)
            for half in range(2):
                w_p1(p, half).start()

        def act_w(p):
            for half in range(2):
                w_p1(p, half).wait()
            ws[p] = wacc[p] + r1[p]
            for half in range(2):
                w_p2(p, half).start()

        def reduced(p):
            for half in range(2):
                w_p2(p, half).wait()
            return ws[p] + r2[p]

        def update(h, slot, p, y):
            for k, part in enumerate(split(-y)):
                yp[k] = part
            t0 = rows // TILE - tiles_of(h)

            def one(t, n):
                for u in range(n):
                    xt[t0 + t + u] += dot6([(tuple(yp[k] for k in range(3)), parts(slot, t + u, pl.ds(256 * p, 256)))], 1, 1)
            over_tiles(tiles_of(h), one)

        last = blocks - 1
        top = rows // TILE - 1
        issue_v(last)
        v_loc(last).start()
        issue_z(top)
        for hh in range(last - 1, last - AHEAD, -1):
            issue_v(hh)
        v_loc(last - 1).start()
        for t in range(top - 1, top - Z_START, -1):
            issue_z(t)
        forward_v(last)
        collect_v(last)
        prepare(last, last % 2)
        gram(last, last % 2)
        for half in range(2):
            g_p1(half).start()
        forward_v(last - 1)

        def block_step(i, _):
            h = last - i
            slot = h % 2
            nslot = 1 - slot

            @pl.when(slot == 1)
            def _():
                collect_z((h - 1) // 2)

            product(h, slot, 1)
            product(h, slot, 0)

            early = h >= SWITCH
            late = h < SWITCH

            @pl.when(early)
            def _():
                act_g()
                act_w(1)

            @pl.when(late)
            def _():
                merge(h, slot)
            for hh in range(blocks - 2):
                @pl.when(h - 2 == hh)
                def _():
                    forward_v(hh)
            for hh in range(blocks - AHEAD):
                @pl.when(h == hh + AHEAD)
                def _():
                    issue_v(hh)
            for hh in range(blocks - 1):
                @pl.when(h - 1 == hh)
                def _():
                    collect_v(hh)

            @pl.when(h > 0)
            def _():
                prepare(h - 1, nslot)
            for hh in range(blocks - 2):
                @pl.when(h - 2 == hh)
                def _():
                    v_loc(hh).start()

            @pl.when(early)
            def _():
                act_w(0)
                merge(h, slot)

            @pl.when(late)
            def _():
                act_w(1)

            @pl.when(h > 0)
            def _():
                gram(h - 1, nslot)

            @pl.when(late)
            def _():
                act_w(0)

            @pl.when(h > 0)
            def _():
                for half in range(2):
                    g_p1(half).start()

            @pl.when(jnp.logical_and(slot == 1, jnp.logical_and(h >= 3, h <= 2 * (top - Z_START) + 3)))
            def _():
                issue_z((h - 3) // 2)
            factor(slot)
            yb = dot(reduced(1), tbuf[slot, 1], 1, 1)
            wacc[1] = dot(yb, nbuf[...], 1, 1)
            update(h, slot, 1, yb)
            ya = dot(reduced(0), tbuf[slot, 0], 1, 1) - wacc[1]

            update(h, slot, 0, ya)

            @pl.when(jnp.logical_and(h > 0, h <= SWITCH))
            def _():
                act_g()
            return 0

        lax.fori_loop(0, blocks, block_step, 0)
        for t in range(rows // TILE):
            o_ref[TILE * t:TILE * t + TILE, :] = xt[t].T
        for hh in range(blocks):
            v_x(hh).wait_send()
            v_sib(hh).wait_send()
            v_fwd(hh).wait_send()
            for cp in t_copies(hh):
                cp.wait_send()
        for t in range(rows // TILE):
            for cp in z_copies(t):
                cp.wait_send()

    return body


def solution(mesh):
    def local(v_loc, t_loc, z_loc):
        rows, cols = v_loc.shape
        blocks = cols // 128
        t_loc = t_loc.reshape(blocks, 2, 64, 64)
        tiles = ((blocks + 1) // 2) * ((blocks + 2) // 2)
        dma = pltpu.SemaphoreType.DMA
        hbm = pl.BlockSpec(memory_space=pl.ANY)
        return pl.pallas_call(
            make_kernel(rows, blocks),
            out_shape=jax.ShapeDtypeStruct((rows, 256), F32),
            in_specs=[hbm] * 3,
            out_specs=pl.BlockSpec(memory_space=pltpu.VMEM),
            scratch_shapes=[
                pltpu.VMEM((3 * TILE * tiles + 2 * rows, 128), F32),
                pltpu.VMEM((2, 3, rows, 512), BF16),
                pltpu.VMEM((4, blocks, 64, 64), F32),
                pltpu.VMEM((rows // TILE, 256, TILE), F32),
                pltpu.VMEM((2, 256, 256), F32), pltpu.VMEM((2, 256, 256), F32),
                pltpu.VMEM((2, 256, 256), F32), pltpu.VMEM((2, 256, 256), F32),
                pltpu.VMEM((3, 256, 256), BF16),
                pltpu.VMEM((384, 256), F32),
                pltpu.VMEM((448, 128), F32), pltpu.VMEM((448, 128), F32),
                pltpu.VMEM((448, 128), F32), pltpu.VMEM((448, 128), F32),
                pltpu.VMEM((2, 2, 256, 256), F32),
                pltpu.VMEM((2, 256, 256), F32),
                pltpu.VMEM((256, 256), F32),
                dma((blocks,)), dma((blocks,)), dma((blocks,)), dma((blocks,)), dma((3, blocks)),
                dma((blocks,)), dma((blocks,)), dma((blocks,)), dma((blocks,)), dma((4, blocks)),
                dma((3, rows // TILE)), dma((rows // TILE,)), dma((4, rows // TILE)),
                dma((2, 2)), dma((2, 2)), dma((2, 2)), dma((2, 2)),
                dma((2,)), dma((2,)), dma((2,)), dma((2,)),
                dma((2, 2)), dma((2, 2)),
            ],
            compiler_params=pltpu.CompilerParams(collective_id=0, has_side_effects=True,
                                                 vmem_limit_bytes=67043328),
        )(v_loc, t_loc, z_loc.T)

    return jax.shard_map(local, mesh=mesh,
                         in_specs=(P('row', 'col'), P('col', None, None), P(None, ('col', 'row'))),
                         out_specs=P('row', 'col'), check_vma=False)
```

```python
import jax
import jax.numpy as jnp
from jax import lax
from jax.experimental import pallas as pl
from jax.experimental.pallas import tpu as pltpu
from jax.sharding import PartitionSpec as P

F32 = jnp.float32
BF16 = jnp.bfloat16
MESH = pl.DeviceIdType.MESH
TILE = 256
AHEAD = 8
Z_START = 3


def dot(a, b, ca, cb):
    return lax.dot_general(a, b, (((ca,), (cb,)), ((), ())), preferred_element_type=F32,
                           precision=lax.Precision.HIGHEST)


def split(a):
    a1 = a.astype(BF16)
    rest = a - a1.astype(F32)
    a2 = rest.astype(BF16)
    return a1, a2, (rest - a2.astype(F32)).astype(BF16)


def dot6(pairs, ca, cb):
    lhs, rhs = [], []
    for (a1, a2, a3), (b1, b2, b3) in pairs:
        lhs += [a3, a1, a2, a1, a2, a1]
        rhs += [b1, b3, b2, b2, b1, b1]
    return lax.dot_general(jnp.concatenate(lhs, ca), jnp.concatenate(rhs, cb), (((ca,), (cb,)), ((), ())),
                           preferred_element_type=F32)


def make_kernel(rows, blocks):
    def tiles_of(h):
        return (blocks + 1 - h) // 2

    def tiles_before(h):
        k = blocks - 1 - h
        return ((k + 1) // 2) * ((k + 2) // 2)

    area = TILE * tiles_before(-1)

    def body(v_hbm, t_hbm, z_hbm, o_hbm, vbuf, vp, tall, xt, wacc, r1, ws, r2, yp, gkk, gacc, gr1, gr2, gf, tbuf, gab,
             nbuf, vx_s, vsib_s, vfwd_s, vloc_s, v_r, tx_s, txc_s, tsib_s, tloc_s, t_r, z_s, zloc_s, z_r,
             p1_s, p1_r, p2_s, p2_r, g_s, g_r, d_s, d_r, o_s):
        r = lax.axis_index("row")
        c = lax.axis_index("col")
        core = c % 2
        cx, csib, cxc = (c + 2) % 4, c + 1 - 2 * core, 3 - c
        ry, rz, rd = r + 1 - 2 * (r % 2), (r + 2) % 4, 3 - r
        dev_x, dev_sib, dev_xc = (r, cx), (r, csib), (r, cxc)
        dev_y, dev_z, dev_d = (ry, c), (rz, c), (rd, c)

        def remote(src, dst, ss, rs, dev):
            return pltpu.make_async_remote_copy(src, dst, ss, rs, device_id=dev, device_id_type=MESH)

        barrier = pltpu.get_barrier_semaphore()
        for dev in (dev_x, dev_sib, dev_xc, dev_y, dev_z, dev_d):
            pl.semaphore_signal(barrier, 1, device_id=dev, device_id_type=MESH)
        pl.semaphore_wait(barrier, 6)

        def v_src(hh):
            n = 128 * (blocks - hh)
            return v_hbm.at[pl.ds(rows - n, n), pl.ds(hh * 128, 128)]

        def v_rows(base, hh):
            return vbuf.at[pl.ds(base + 128 * (hh % 2), 128 * (blocks - hh)), :]

        def v_dst(rel, hh):
            return v_rows(area * (rel - 1) + TILE * tiles_before(hh), hh)

        def v_x(hh):
            return remote(v_src(hh), v_dst(2, hh), vx_s.at[hh], v_r.at[1, hh], dev_x)

        def v_sib(hh):
            return remote(v_src(hh), v_dst(1, hh), vsib_s.at[hh], v_r.at[0, hh], dev_sib)

        def v_fwd(hh):
            return remote(v_dst(2, hh), v_dst(3, hh), vfwd_s.at[hh], v_r.at[2, hh], dev_sib)

        def v_loc(hh):
            return pltpu.make_async_copy(v_src(hh), v_rows(3 * area + rows * (hh % 2), hh), vloc_s.at[hh])

        def clear_v():
            for rel in range(3):
                for hh in range(1, blocks, 2):
                    vbuf[pl.ds(area * rel + TILE * tiles_before(hh), 128), :] = jnp.zeros((128, 128), F32)
            vbuf[pl.ds(3 * area + rows, 128), :] = jnp.zeros((128, 128), F32)

        def v_arrive(rel, hh):
            return remote(v_src(hh), v_dst(rel, hh), vx_s.at[hh], v_r.at[rel - 1, hh], dev_x)

        def t_copies(h):
            return (remote(t_hbm.at[h, core], tall.at[c, h], tx_s.at[h], t_r.at[c, h], dev_x),
                    remote(t_hbm.at[h, 1 - core], tall.at[c, h], txc_s.at[h], t_r.at[c, h], dev_xc),
                    remote(t_hbm.at[h, 1 - core], tall.at[c, h], tsib_s.at[h], t_r.at[c, h], dev_sib))

        def t_loc(h):
            return pltpu.make_async_copy(t_hbm.at[h, core], tall.at[c, h], tloc_s.at[h])

        def t_arrive(slot, h):
            return remote(t_hbm.at[h, core], tall.at[slot, h], tx_s.at[h], t_r.at[slot, h], dev_x)

        def issue_v(hh):
            for cp in t_copies(hh):
                cp.start()
            t_loc(hh).start()
            v_x(hh).start()
            v_sib(hh).start()

        def forward_v(hh):
            v_arrive(2, hh).wait_recv()
            v_fwd(hh).start()

        def collect_v(hh):
            v_loc(hh).wait()
            v_arrive(1, hh).wait_recv()
            v_arrive(3, hh).wait_recv()
            t_loc(hh).wait()
            for slot in (cx, csib, cxc):
                t_arrive(slot, hh).wait_recv()

        def z_src(to, t):
            return z_hbm.at[:, pl.ds(pl.multiple_of(rows * to + TILE * t, TILE), TILE)]

        def z_dst(src_r, t):
            return xt.at[t, pl.ds(pl.multiple_of(64 * src_r, 64), 64), :]

        def z_copies(t):
            return [remote(z_src(dev[0], t), z_dst(r, t), z_s.at[i, t], z_r.at[r, t], dev)
                    for i, dev in enumerate((dev_y, dev_z, dev_d))]

        def z_loc(t):
            return pltpu.make_async_copy(z_src(r, t), z_dst(r, t), zloc_s.at[t])

        def issue_z(t):
            for cp in z_copies(t):
                cp.start()
            z_loc(t).start()

        def collect_z(t):
            z_loc(t).wait()
            for src_r in (ry, rz, rd):
                remote(z_src(r, t), z_dst(src_r, t), z_s.at[0, t], z_r.at[src_r, t], dev_y).wait_recv()

        def steps(half):
            return (dev_y, dev_z) if half == 0 else (dev_z, dev_y)

        def w_p1(p, half):
            s = pl.ds(128 * half, 128)
            return remote(wacc.at[p, s], r1.at[p, s], p1_s.at[p, half], p1_r.at[p, half], steps(half)[0])

        def w_p2(p, half):
            s = pl.ds(128 * half, 128)
            return remote(ws.at[p, s], r2.at[p, s], p2_s.at[p, half], p2_r.at[p, half], steps(half)[1])

        def g_place(f):
            k1, k2 = ((r % 2), (r // 2)) if f == 0 else ((r // 2), (r % 2))
            return 224 * f, k1, k2

        def g_rows(start, n):
            return pl.ds(pl.multiple_of(start, 8), n)

        def g_rs1(par, f):
            base, k1, _ = g_place(f)
            s = g_rows(base + 112 * (1 - k1), 112)
            return remote(gacc.at[par, s], gr1.at[par, s], g_s.at[0, par, f], g_r.at[0, par, f], steps(f)[0])

        def g_rs2(par, f):
            base, k1, k2 = g_place(f)
            s = g_rows(base + 112 * k1 + 56 * (1 - k2), 56)
            return remote(gacc.at[par, s], gr2.at[par, s], g_s.at[1, par, f], g_r.at[1, par, f], steps(f)[1])

        def g_ag2(par, f):
            base, k1, k2 = g_place(f)
            s = g_rows(base + 112 * k1 + 56 * k2, 56)
            return remote(gf.at[par, s], gf.at[par, s], g_s.at[2, par, f], g_r.at[2, par, f], steps(f)[1])

        def g_ag1(par, f):
            base, k1, _ = g_place(f)
            s = g_rows(base + 112 * k1, 112)
            return remote(gf.at[par, s], gf.at[par, s], g_s.at[3, par, f], g_r.at[3, par, f], steps(f)[0])

        def act_rs2(par):
            for f in range(2):
                base, k1, _ = g_place(f)
                g_rs1(par, f).wait()
                s = g_rows(base + 112 * k1, 112)
                gacc[par, s] = gacc[par, s] + gr1[par, s]
                g_rs2(par, f).start()

        def act_ag2(par):
            for f in range(2):
                base, k1, k2 = g_place(f)
                g_rs2(par, f).wait()
                s = g_rows(base + 112 * k1 + 56 * k2, 56)
                gf[par, s] = gacc[par, s] + gr2[par, s]
                g_ag2(par, f).start()

        def act_ag1(par):
            for f in range(2):
                g_ag2(par, f).wait()
                g_ag1(par, f).start()

        def over_tiles(n, fn):
            def four(t, _):
                fn(4 * t, 4)
                return 0
            lax.fori_loop(0, n // 4, four, 0)

            @pl.when(n % 4 >= 2)
            def _():
                fn(4 * (n // 4), 2)

            @pl.when(n % 2 == 1)
            def _():
                fn(n - 1, 1)

        def whole(n, fn):
            for k in range(1, rows // TILE + 1):
                @pl.when(n == k)
                def _():
                    fn(0, k)

        def prepare(h, slot):
            bases = []
            for i in range(4):
                rel = ((c // 2 + i // 2) % 2) * 2 + (c + i) % 2
                own = (3 - rel) // 3
                bases.append(own * (3 * area + rows * (h % 2)) + (1 - own) * (area * (rel - 1) + TILE * tiles_before(h)))

            def one(t, _):
                d = pl.ds(pl.multiple_of(TILE * t, TILE), TILE)
                for i in range(2):
                    a = vbuf[pl.ds(pl.multiple_of(bases[2 * i] + TILE * t, TILE), TILE), :]
                    b = vbuf[pl.ds(pl.multiple_of(bases[2 * i + 1] + TILE * t, TILE), TILE), :]
                    low = lax.broadcasted_iota(jnp.int32, a.shape, 1) < 64
                    ar, br = pltpu.roll(a, 64, 1), pltpu.roll(b, 64, 1)
                    for k, part in enumerate(split(jnp.where(low, a, br))):
                        vp[slot, k, d, 128 * i:128 * i + 128] = part
                    for k, part in enumerate(split(jnp.where(low, ar, b))):
                        vp[slot, k, d, 256 + 128 * i:256 + 128 * i + 128] = part
                return 0
            lax.fori_loop(0, tiles_of(h), one, 0)

        def parts(slot, t, lanes):
            s = pl.ds(pl.multiple_of(TILE * t, TILE), TILE)
            return tuple(vp[slot, k, s, lanes] for k in range(3))

        def gram(h, slot):
            gkk[...] = jnp.zeros_like(gkk)
            mine = pl.ds(pl.multiple_of(256 * core, 256), 256)
            half = pl.ds(pl.multiple_of(128 * core, 128), 128)

            def one(t, n):
                own = [parts(slot, t + u, mine) for u in range(n)]
                gkk[0:256, :] += dot6([(a, a) for a in own], 0, 0)
                gkk[256:384, :] += dot6([(parts(slot, t + u, half), parts(slot, t + u, pl.ds(256, 256)))
                                         for u in range(n)], 0, 0)
            over_tiles(tiles_of(h), one)

        def send_g(par):
            gacc[par, 0:128, :] = gkk[256:384, 0:128]
            gacc[par, 128:256, :] = gkk[256:384, 128:256]
            gacc[par, 256:384, :] = gkk[0:128, 128:256]
            gacc[par, 384:448, 0:64] = gkk[0:64, 64:128]
            gacc[par, 384:448, 64:128] = gkk[128:192, 192:256]
            for f in range(2):
                g_rs1(par, f).start()

        def rows_of(k):
            return pl.ds(pl.multiple_of(128 * k, 128), 128)

        def share(slot, k):
            return (remote(tbuf.at[slot, k], tbuf.at[slot, k], d_s.at[slot, 0], d_r.at[slot, 0], dev_sib),
                    remote(gab.at[slot, rows_of(k)], gab.at[slot, rows_of(k)], d_s.at[slot, 1], d_r.at[slot, 1], dev_sib))

        def merge(h, slot):
            for f in range(2):
                g_ag1(slot, f).wait()
            g = gf[slot]
            gab[slot, rows_of(core), 0:128] = g[0:128]
            gab[slot, rows_of(core), 128:256] = g[128:256]
            zero = jnp.zeros((64, 64), F32)

            def diag(a, b):
                return jnp.concatenate([jnp.concatenate([a, zero], 1), jnp.concatenate([zero, b], 1)], 0)
            t0, t1, t2, t3 = (tall[i, h] for i in range(4))
            low = g[384:448]
            off = dot(diag(low[:, 0:64], low[:, 64:128]), diag(t1, t3), 1, 0)
            off = -dot(diag(t0, t2), off, 1, 0)
            ta = jnp.concatenate([jnp.concatenate([t0, off[0:64, 0:64]], 1), jnp.concatenate([zero, t1], 1)], 0)
            tb = jnp.concatenate([jnp.concatenate([t2, off[64:128, 64:128]], 1), jnp.concatenate([zero, t3], 1)], 0)
            cross = -dot(ta, dot(g[256:384], tb, 1, 0), 1, 0)
            tbuf[slot, core, 0:128, 0:128] = ta
            tbuf[slot, core, 0:128, 128:256] = cross
            tbuf[slot, core, 128:256, 0:128] = jnp.zeros((128, 128), F32)
            tbuf[slot, core, 128:256, 128:256] = tb
            for cp in share(slot, core):
                cp.start()

        def factor(slot):
            for cp in share(slot, core):
                cp.wait_send()
            for cp in share(slot, 1 - core):
                cp.wait_recv()
            tb = tbuf[slot, 1]
            nbuf[0:256, :] = tb
            nbuf[256:512, :] = dot(dot(tbuf[slot, 0], gab[slot], 1, 0), tb, 1, 0)

        def product(h, slot, p, only=0):
            wacc[p] = jnp.zeros((256, 256), F32)
            t0 = rows // TILE - tiles_of(h)

            def one(t, n):
                wacc[p] += dot6([(split(xt[t0 + t + u]), parts(slot, t + u, pl.ds(256 * p, 256)))
                                 for u in range(n)], 1, 0)
            if only:
                one(0, only)
            else:
                whole(tiles_of(h), one)
            for half in range(2):
                w_p1(p, half).start()

        def act_w(p):
            for half in range(2):
                w_p1(p, half).wait()
            ws[p] = wacc[p] + r1[p]
            for half in range(2):
                w_p2(p, half).start()

        def reduced(p):
            for half in range(2):
                w_p2(p, half).wait()
            return ws[p] + r2[p]

        def update(h, slot, p, y):
            for k, part in enumerate(split(-y)):
                yp[k] = part
            t0 = rows // TILE - tiles_of(h)

            def one(t, n):
                for u in range(n):
                    xt[t0 + t + u] += dot6([(tuple(yp[k] for k in range(3)), parts(slot, t + u, pl.ds(256 * p, 256)))], 1, 1)
            whole(tiles_of(h), one)

        def ready(h, slot):
            collect_v(h)
            prepare(h, slot)
            gram(h, slot)

        last = blocks - 1
        top = rows // TILE - 1
        issue_v(last)
        v_loc(last).start()
        issue_z(top)
        for hh in range(last - 1, last - AHEAD, -1):
            issue_v(hh)
        v_loc(last - 1).start()
        for t in range(top - 1, top - Z_START, -1):
            issue_z(t)
        clear_v()
        forward_v(last)
        ready(last, last % 3)
        send_g(last % 2)
        collect_z(top)
        for p in (1, 0):
            product(last, last % 3, p, only=1)
        forward_v(last - 1)
        v_loc(last - 2).start()
        ready(last - 1, (last - 1) % 3)
        act_rs2(last % 2)
        send_g((last - 1) % 2)
        act_w(1)
        act_ag2(last % 2)
        act_w(0)
        act_ag1(last % 2)
        act_rs2((last - 1) % 2)
        forward_v(last - 2)

        def block_step(i, _):
            h = last - i
            slot = h % 2
            vslot = h % 3

            @pl.when(jnp.logical_and(slot == 1, h < last))
            def _():
                collect_z((h - 1) // 2)

            @pl.when(h < last)
            def _():
                product(h, vslot, 1)
                product(h, vslot, 0)
            merge(h, slot)

            @pl.when(jnp.logical_and(h > 0, h < last))
            def _():
                act_rs2(1 - slot)
            for hh in range(blocks - 3):
                @pl.when(h - 3 == hh)
                def _():
                    forward_v(hh)
            for hh in range(blocks - AHEAD):
                @pl.when(h == hh + AHEAD)
                def _():
                    issue_v(hh)
            for hh in range(blocks - 2):
                @pl.when(h - 2 == hh)
                def _():
                    collect_v(hh)

            @pl.when(h > 1)
            def _():
                prepare(h - 2, (h - 2) % 3)
            for hh in range(blocks - 3):
                @pl.when(h - 3 == hh)
                def _():
                    v_loc(hh).start()
            @pl.when(h < last)
            def _():
                act_w(1)

            @pl.when(h > 1)
            def _():
                gram(h - 2, (h - 2) % 3)

            @pl.when(h < last)
            def _():
                act_w(0)

            @pl.when(h > 0)
            def _():
                act_ag2(1 - slot)

            @pl.when(h > 1)
            def _():
                send_g(slot)

            @pl.when(jnp.logical_and(slot == 1, jnp.logical_and(h >= 3, h <= 2 * (top - Z_START) + 3)))
            def _():
                issue_z((h - 3) // 2)
            factor(slot)
            yb = dot(reduced(1), nbuf[...], 1, 1)
            wacc[1] = yb[:, 256:512]
            update(h, vslot, 1, yb[:, 0:256])
            ya = dot(reduced(0), tbuf[slot, 0], 1, 1) - wacc[1]
            update(h, vslot, 0, ya)

            @pl.when(h > 0)
            def _():
                act_ag1(1 - slot)
            return 0

        lax.fori_loop(0, blocks, block_step, 0)
        stages = [buf.at[k] for buf in (wacc, r1, ws, r2) for k in range(2)]
        outs = []
        for t in range(rows // TILE):
            if t >= len(stages):
                outs[t - len(stages)].wait()
            stages[t % len(stages)][...] = xt[t].T
            outs.append(pltpu.make_async_copy(stages[t % len(stages)], o_hbm.at[pl.ds(TILE * t, TILE), :], o_s.at[t]))
            outs[t].start()
        for cp in outs[-len(stages):]:
            cp.wait()
        for hh in range(blocks):
            v_x(hh).wait_send()
            v_sib(hh).wait_send()
            v_fwd(hh).wait_send()
            for cp in t_copies(hh):
                cp.wait_send()
        for t in range(rows // TILE):
            for cp in z_copies(t):
                cp.wait_send()

    return body


def solution(mesh):
    def local(v_loc, t_loc, z_loc):
        rows, cols = v_loc.shape
        blocks = cols // 128
        t_loc = t_loc.reshape(blocks, 2, 64, 64)
        tiles = ((blocks + 1) // 2) * ((blocks + 2) // 2)
        dma = pltpu.SemaphoreType.DMA
        hbm = pl.BlockSpec(memory_space=pl.ANY)
        return pl.pallas_call(
            make_kernel(rows, blocks),
            out_shape=jax.ShapeDtypeStruct((rows, 256), F32),
            in_specs=[hbm] * 3,
            out_specs=hbm,
            scratch_shapes=[
                pltpu.VMEM((3 * TILE * tiles + 2 * rows, 128), F32),
                pltpu.VMEM((3, 3, rows, 512), BF16),
                pltpu.VMEM((4, blocks, 64, 64), F32),
                pltpu.VMEM((rows // TILE, 256, TILE), F32),
                pltpu.VMEM((2, 256, 256), F32), pltpu.VMEM((2, 256, 256), F32),
                pltpu.VMEM((2, 256, 256), F32), pltpu.VMEM((2, 256, 256), F32),
                pltpu.VMEM((3, 256, 256), BF16),
                pltpu.VMEM((384, 256), F32),
                pltpu.VMEM((2, 448, 128), F32), pltpu.VMEM((2, 448, 128), F32),
                pltpu.VMEM((2, 448, 128), F32), pltpu.VMEM((2, 448, 128), F32),
                pltpu.VMEM((2, 2, 256, 256), F32),
                pltpu.VMEM((2, 256, 256), F32),
                pltpu.VMEM((512, 256), F32),
                dma((blocks,)), dma((blocks,)), dma((blocks,)), dma((blocks,)), dma((3, blocks)),
                dma((blocks,)), dma((blocks,)), dma((blocks,)), dma((blocks,)), dma((4, blocks)),
                dma((3, rows // TILE)), dma((rows // TILE,)), dma((4, rows // TILE)),
                dma((2, 2)), dma((2, 2)), dma((2, 2)), dma((2, 2)),
                dma((4, 2, 2)), dma((4, 2, 2)),
                dma((2, 2)), dma((2, 2)), dma((rows // TILE,)),
            ],
            compiler_params=pltpu.CompilerParams(collective_id=0, has_side_effects=True,
                                                 vmem_limit_bytes=67043328),
        )(v_loc, t_loc, z_loc.T)

    return jax.shard_map(local, mesh=mesh,
                         in_specs=(P('row', 'col'), P('col', None, None), P(None, ('col', 'row'))),
                         out_specs=P('row', 'col'), check_vma=False)
```

```python
import jax
import jax.numpy as jnp
from jax import lax
from jax.experimental import pallas as pl
from jax.experimental.pallas import tpu as pltpu
from jax.sharding import PartitionSpec as P

F32 = jnp.float32
BF16 = jnp.bfloat16
MESH = pl.DeviceIdType.MESH
TILE = 256
AHEAD = 8
GATHER = 8


def dot(a, b, ca, cb):
    return lax.dot_general(a, b, (((ca,), (cb,)), ((), ())), preferred_element_type=F32,
                           precision=lax.Precision.HIGHEST)


def split(a):
    a1 = a.astype(BF16)
    rest = a - a1.astype(F32)
    a2 = rest.astype(BF16)
    return a1, a2, (rest - a2.astype(F32)).astype(BF16)


def dot6(pairs, ca, cb):
    lhs, rhs = [], []
    for (a1, a2, a3), (b1, b2, b3) in pairs:
        lhs += [a3, a1, a2, a1, a2, a1]
        rhs += [b1, b3, b2, b2, b1, b1]
    return lax.dot_general(jnp.concatenate(lhs, ca), jnp.concatenate(rhs, cb), (((ca,), (cb,)), ((), ())),
                           preferred_element_type=F32)


def make_kernel(rows, blocks):
    def tiles_of(h):
        return (blocks + 1 - h) // 2

    def tiles_before(h):
        k = blocks - 1 - h
        return ((k + 1) // 2) * ((k + 2) // 2)

    area = TILE * tiles_before(-1)

    def body(v_hbm, t_hbm, z_hbm, o_hbm, vbuf, vp, tall, xt, wacc, r1, ws, r2, yp, gkk, gacc, gr1, gr2, gf, tbuf, gab,
             nbuf, vx_s, vsib_s, vfwd_s, vloc_s, v_r, tx_s, txc_s, tsib_s, tloc_s, t_r, z_s, zloc_s, z_r,
             p1_s, p1_r, p2_s, p2_r, g_s, g_r, w_s, w_r, d_s, d_r, o_s):
        r = lax.axis_index("row")
        c = lax.axis_index("col")
        core = c % 2
        cx, csib, cxc = (c + 2) % 4, c + 1 - 2 * core, 3 - c
        ry, rz, rd = r + 1 - 2 * (r % 2), (r + 2) % 4, 3 - r
        dev_x, dev_sib, dev_xc = (r, cx), (r, csib), (r, cxc)
        dev_y, dev_z, dev_d = (ry, c), (rz, c), (rd, c)

        last = blocks - 1

        def remote(src, dst, ss, rs, dev):
            return pltpu.make_async_remote_copy(src, dst, ss, rs, device_id=dev, device_id_type=MESH)

        barrier = pltpu.get_barrier_semaphore()
        for dev in (dev_x, dev_sib, dev_xc, dev_y, dev_z, dev_d):
            pl.semaphore_signal(barrier, 1, device_id=dev, device_id_type=MESH)
        pl.semaphore_wait(barrier, 6)

        def v_src(hh):
            n = 128 * (blocks - hh)
            return v_hbm.at[pl.ds(rows - n, n), pl.ds(hh * 128, 128)]

        def v_rows(base, hh):
            return vbuf.at[pl.ds(base + 128 * (hh % 2), 128 * (blocks - hh)), :]

        def v_dst(rel, hh):
            return v_rows(area * (rel - 1) + TILE * tiles_before(hh), hh)

        def v_x(hh):
            return remote(v_src(hh), v_dst(2, hh), vx_s.at[hh], v_r.at[1, hh], dev_x)

        def v_sib(hh):
            return remote(v_src(hh), v_dst(1, hh), vsib_s.at[hh], v_r.at[0, hh], dev_sib)

        def v_fwd(hh):
            return remote(v_dst(2, hh), v_dst(3, hh), vfwd_s.at[hh], v_r.at[2, hh], dev_sib)

        def v_loc(hh):
            return pltpu.make_async_copy(v_src(hh), v_rows(3 * area + rows * (hh % 2), hh), vloc_s.at[hh])

        def clear_v():
            for rel in range(3):
                for hh in range(1, blocks, 2):
                    vbuf[pl.ds(area * rel + TILE * tiles_before(hh), 128), :] = jnp.zeros((128, 128), F32)
            vbuf[pl.ds(3 * area + rows, 128), :] = jnp.zeros((128, 128), F32)

        def v_arrive(rel, hh):
            return remote(v_src(hh), v_dst(rel, hh), vx_s.at[hh], v_r.at[rel - 1, hh], dev_x)

        def t_copies(h):
            return (remote(t_hbm.at[h, core], tall.at[c, h], tx_s.at[h], t_r.at[c, h], dev_x),
                    remote(t_hbm.at[h, 1 - core], tall.at[c, h], txc_s.at[h], t_r.at[c, h], dev_xc),
                    remote(t_hbm.at[h, 1 - core], tall.at[c, h], tsib_s.at[h], t_r.at[c, h], dev_sib))

        def t_loc(h):
            return pltpu.make_async_copy(t_hbm.at[h, core], tall.at[c, h], tloc_s.at[h])

        def t_arrive(slot, h):
            return remote(t_hbm.at[h, core], tall.at[slot, h], tx_s.at[h], t_r.at[slot, h], dev_x)

        def issue_v(hh):
            v_x(hh).start()
            v_sib(hh).start()
            for cp in t_copies(hh):
                cp.start()
            t_loc(hh).start()

        def forward_v(hh):
            v_arrive(2, hh).wait_recv()
            v_fwd(hh).start()

        def collect_v(hh):
            v_loc(hh).wait()
            v_arrive(1, hh).wait_recv()
            v_arrive(3, hh).wait_recv()
            t_loc(hh).wait()
            for slot in (cx, csib, cxc):
                t_arrive(slot, hh).wait_recv()

        def z_src(to, t, part):
            return z_hbm.at[:, pl.ds(pl.multiple_of(rows * to + TILE * t + 128 * part, 128), 128)]

        def z_dst(src_r, t, part):
            return xt.at[t, pl.ds(pl.multiple_of(64 * src_r, 64), 64), pl.ds(128 * part, 128)]

        def z_copies(t, part):
            return [remote(z_src(dev[0], t, part), z_dst(r, t, part), z_s.at[i, t, part], z_r.at[r, t, part], dev)
                    for i, dev in enumerate((dev_y, dev_z, dev_d))]

        def z_loc(t, part):
            return pltpu.make_async_copy(z_src(r, t, part), z_dst(r, t, part), zloc_s.at[t, part])

        def issue_z(t, part):
            for cp in z_copies(t, part):
                cp.start()
            z_loc(t, part).start()

        def collect_z(t):
            for part in range(2):
                z_loc(t, part).wait()
                for src_r in (ry, rz, rd):
                    dst = z_dst(src_r, t, part)
                    remote(z_src(r, t, part), dst, z_s.at[0, t, part], z_r.at[src_r, t, part], dev_y).wait_recv()

        def steps(half):
            return (dev_y, dev_z) if half == 0 else (dev_z, dev_y)

        def w_p1(p, half):
            s = pl.ds(128 * half, 128)
            return remote(wacc.at[p, s], r1.at[p, s], p1_s.at[p, half], p1_r.at[p, half], steps(half)[0])

        def w_p2(p, half):
            s = pl.ds(128 * half, 128)
            return remote(ws.at[p, s], r2.at[p, s], p2_s.at[p, half], p2_r.at[p, half], steps(half)[1])

        def g_place(f):
            k1, k2 = ((r % 2), (r // 2)) if f == 0 else ((r // 2), (r % 2))
            return 224 * f, k1, k2

        def g_rows(start, n):
            return pl.ds(pl.multiple_of(start, 8), n)

        def w_kept(f, other=0):
            k1 = r % 2 if f == 0 else r // 2
            return g_rows(128 * f + 64 * (k1 + other * (1 - 2 * k1)), 64)

        def w_e1(p, f):
            s = w_kept(f, 1)
            return remote(wacc.at[p, s], r1.at[p, s], w_s.at[0, p, f], w_r.at[0, p, f], steps(f)[0])

        def w_e2(p, f):
            s = w_kept(f)
            return remote(ws.at[p, s], r2.at[p, s], w_s.at[1, p, f], w_r.at[1, p, f], steps(f)[1])

        def w_e3(p, f):
            s = w_kept(f)
            return remote(wacc.at[p, s], wacc.at[p, s], w_s.at[2, p, f], w_r.at[2, p, f], steps(f)[0])

        def w_act1(p):
            for f in range(2):
                w_e1(p, f).wait()
            for f in range(2):
                s = w_kept(f)
                ws[p, s] = wacc[p, s] + r1[p, s]
                w_e2(p, f).start()

        def w_act2(p):
            for f in range(2):
                w_e2(p, f).wait()
            for f in range(2):
                s = w_kept(f)
                wacc[p, s] = ws[p, s] + r2[p, s]
                w_e3(p, f).start()

        def g_p1(par, f):
            s = pl.ds(224 * f, 224)
            return remote(gacc.at[par, s], gr1.at[par, s], g_s.at[0, par, f], g_r.at[0, par, f], steps(f)[0])

        def g_p2(par, f):
            s = pl.ds(224 * f, 224)
            return remote(gacc.at[par, s], gr2.at[par, s], g_s.at[1, par, f], g_r.at[1, par, f], steps(f)[1])

        def act_p2(par):
            for f in range(2):
                g_p1(par, f).wait()
            gacc[par] = gacc[par] + gr1[par]
            for f in range(2):
                g_p2(par, f).start()

        def g_rs1(par, f):
            base, k1, _ = g_place(f)
            s = g_rows(base + 112 * (1 - k1), 112)
            return remote(gacc.at[par, s], gr1.at[par, s], g_s.at[0, par, f], g_r.at[0, par, f], steps(f)[0])

        def g_rs2(par, f):
            base, k1, k2 = g_place(f)
            s = g_rows(base + 112 * k1 + 56 * (1 - k2), 56)
            return remote(gacc.at[par, s], gr2.at[par, s], g_s.at[1, par, f], g_r.at[1, par, f], steps(f)[1])

        def g_ag2(par, f):
            base, k1, k2 = g_place(f)
            s = g_rows(base + 112 * k1 + 56 * k2, 56)
            return remote(gf.at[par, s], gf.at[par, s], g_s.at[2, par, f], g_r.at[2, par, f], steps(f)[1])

        def g_ag1(par, f):
            base, k1, _ = g_place(f)
            s = g_rows(base + 112 * k1, 112)
            return remote(gf.at[par, s], gf.at[par, s], g_s.at[3, par, f], g_r.at[3, par, f], steps(f)[0])

        def act_rs2(par):
            for f in range(2):
                g_rs1(par, f).wait()
            for f in range(2):
                base, k1, _ = g_place(f)
                s = g_rows(base + 112 * k1, 112)
                gacc[par, s] = gacc[par, s] + gr1[par, s]
                g_rs2(par, f).start()

        def act_ag2(par):
            for f in range(2):
                base, k1, k2 = g_place(f)
                g_rs2(par, f).wait()
                s = g_rows(base + 112 * k1 + 56 * k2, 56)
                gf[par, s] = gacc[par, s] + gr2[par, s]
                g_ag2(par, f).start()

        def act_ag1(par):
            for f in range(2):
                g_ag2(par, f).wait()
                g_ag1(par, f).start()

        def over_tiles(n, fn):
            def four(t, _):
                fn(4 * t, 4)
                return 0
            lax.fori_loop(0, n // 4, four, 0)

            @pl.when(n % 4 >= 2)
            def _():
                fn(4 * (n // 4), 2)

            @pl.when(n % 2 == 1)
            def _():
                fn(n - 1, 1)

        def whole(n, fn):
            for k in range(1, rows // TILE + 1):
                @pl.when(n == k)
                def _():
                    fn(0, k)

        def prepare(h, slot):
            bases = []
            for i in range(4):
                rel = ((c // 2 + i // 2) % 2) * 2 + (c + i) % 2
                own = (3 - rel) // 3
                bases.append(own * (3 * area + rows * (h % 2)) + (1 - own) * (area * (rel - 1) + TILE * tiles_before(h)))

            def one(t, _):
                d = pl.ds(pl.multiple_of(TILE * t, TILE), TILE)
                for i in range(2):
                    a = vbuf[pl.ds(pl.multiple_of(bases[2 * i] + TILE * t, TILE), TILE), :]
                    b = vbuf[pl.ds(pl.multiple_of(bases[2 * i + 1] + TILE * t, TILE), TILE), :]
                    low = lax.broadcasted_iota(jnp.int32, a.shape, 1) < 64
                    ar, br = pltpu.roll(a, 64, 1), pltpu.roll(b, 64, 1)
                    for k, part in enumerate(split(jnp.where(low, a, br))):
                        vp[slot, k, d, 128 * i:128 * i + 128] = part
                    for k, part in enumerate(split(jnp.where(low, ar, b))):
                        vp[slot, k, d, 256 + 128 * i:256 + 128 * i + 128] = part
                return 0
            lax.fori_loop(0, tiles_of(h), one, 0)

        def parts(slot, t, lanes):
            s = pl.ds(pl.multiple_of(TILE * t, TILE), TILE)
            return tuple(vp[slot, k, s, lanes] for k in range(3))

        def gram(h, slot):
            gkk[...] = jnp.zeros_like(gkk)
            mine = pl.ds(pl.multiple_of(256 * core, 256), 256)
            half = pl.ds(pl.multiple_of(128 * core, 128), 128)

            def one(t, n):
                own = [parts(slot, t + u, mine) for u in range(n)]
                gkk[0:256, :] += dot6([(a, a) for a in own], 0, 0)
                gkk[256:384, :] += dot6([(parts(slot, t + u, half), parts(slot, t + u, pl.ds(256, 256)))
                                         for u in range(n)], 0, 0)
            over_tiles(tiles_of(h), one)

        def send_g(par, first=g_rs1):
            gacc[par, 0:128, :] = gkk[256:384, 0:128]
            gacc[par, 128:256, :] = gkk[256:384, 128:256]
            gacc[par, 256:384, :] = gkk[0:128, 128:256]
            gacc[par, 384:448, 0:64] = gkk[0:64, 64:128]
            gacc[par, 384:448, 64:128] = gkk[128:192, 192:256]
            for f in range(2):
                first(par, f).start()

        def rows_of(k):
            return pl.ds(pl.multiple_of(128 * k, 128), 128)

        def share(slot, k):
            return (remote(tbuf.at[slot, k], tbuf.at[slot, k], d_s.at[slot, 0], d_r.at[slot, 0], dev_sib),
                    remote(gab.at[slot, rows_of(k)], gab.at[slot, rows_of(k)], d_s.at[slot, 1], d_r.at[slot, 1], dev_sib))

        def merge(h, slot):
            @pl.when(h >= last - 1)
            def _():
                for f in range(2):
                    g_p2(slot, f).wait()
                gf[slot] = gacc[slot] + gr2[slot]

            @pl.when(h < last - 1)
            def _():
                for f in range(2):
                    g_ag1(slot, f).wait()
            g = gf[slot]
            gab[slot, rows_of(core), 0:128] = g[0:128]
            gab[slot, rows_of(core), 128:256] = g[128:256]
            zero = jnp.zeros((64, 64), F32)

            def diag(a, b):
                return jnp.concatenate([jnp.concatenate([a, zero], 1), jnp.concatenate([zero, b], 1)], 0)
            t0, t1, t2, t3 = (tall[i, h] for i in range(4))
            low = g[384:448]
            off = dot(diag(low[:, 0:64], low[:, 64:128]), diag(t1, t3), 1, 0)
            off = -dot(diag(t0, t2), off, 1, 0)
            ta = jnp.concatenate([jnp.concatenate([t0, off[0:64, 0:64]], 1), jnp.concatenate([zero, t1], 1)], 0)
            tb = jnp.concatenate([jnp.concatenate([t2, off[64:128, 64:128]], 1), jnp.concatenate([zero, t3], 1)], 0)
            cross = -dot(ta, dot(g[256:384], tb, 1, 0), 1, 0)
            tbuf[slot, core, 0:128, 0:128] = ta
            tbuf[slot, core, 0:128, 128:256] = cross
            tbuf[slot, core, 128:256, 0:128] = jnp.zeros((128, 128), F32)
            tbuf[slot, core, 128:256, 128:256] = tb
            for cp in share(slot, core):
                cp.start()

        def factor(slot):
            for cp in share(slot, core):
                cp.wait_send()
            for cp in share(slot, 1 - core):
                cp.wait_recv()
            tb = tbuf[slot, 1]
            nbuf[0:256, :] = tb
            nbuf[256:512, :] = dot(dot(tbuf[slot, 0], gab[slot], 1, 0), tb, 1, 0)

        def gathered(h):
            return jnp.logical_and(h >= GATHER, h < last)

        def pairwise(h):
            return jnp.logical_or(h < GATHER, h == last)

        def product(h, slot, run):
            t0 = rows // TILE - tiles_of(h)

            def group(i, _):
                p = 1 - i
                wacc[p] = jnp.zeros((256, 256), F32)
                lanes = pl.ds(pl.multiple_of(256 * p, 256), 256)

                def one(t, n):
                    wacc[p] += dot6([(split(xt[t0 + t + u]), parts(slot, t + u, lanes)) for u in range(n)], 1, 0)
                run(tiles_of(h), one)
                if run is whole:
                    @pl.when(gathered(h))
                    def _():
                        for f in range(2):
                            w_e1(p, f).start()

                    @pl.when(h < GATHER)
                    def _():
                        for half in range(2):
                            w_p1(p, half).start()
                else:
                    for half in range(2):
                        w_p1(p, half).start()
                return 0
            lax.fori_loop(0, 2, group, 0)

        def act_w(p):
            for half in range(2):
                w_p1(p, half).wait()
            ws[p] = wacc[p] + r1[p]
            for half in range(2):
                w_p2(p, half).start()

        def reduced(h, p):
            @pl.when(gathered(h))
            def _():
                for f in range(2):
                    w_e3(p, f).wait()

            @pl.when(pairwise(h))
            def _():
                for half in range(2):
                    w_p2(p, half).wait()
                wacc[p] = ws[p] + r2[p]
            return wacc[p]

        def update(h, slot, p, y):
            for k, part in enumerate(split(-y)):
                yp[k] = part
            t0 = rows // TILE - tiles_of(h)

            def one(t, n):
                for u in range(n):
                    xt[t0 + t + u] += dot6([(tuple(yp[k] for k in range(3)), parts(slot, t + u, pl.ds(256 * p, 256)))], 1, 1)
            whole(tiles_of(h), one)

        def ready(h, slot):
            collect_v(h)
            prepare(h, slot)
            gram(h, slot)

        def ready(h, slot):
            collect_v(h)
            prepare(h, slot)
            gram(h, slot)

        top = rows // TILE - 1
        issue_v(last)
        v_loc(last).start()
        for part in range(2):
            issue_z(top, part)
        for hh in range(last - 1, last - AHEAD, -1):
            issue_v(hh)
        v_loc(last - 1).start()
        for part in range(2):
            issue_z(top - 1, part)
        clear_v()
        forward_v(last)
        ready(last, last % 3)
        send_g(last % 2, g_p1)
        collect_z(top)
        product(last, last % 3, lambda n, fn: fn(0, 1))
        forward_v(last - 1)
        v_loc(last - 2).start()
        ready(last - 1, (last - 1) % 3)
        act_p2(last % 2)
        act_w(1)
        act_w(0)
        send_g((last - 1) % 2, g_p1)
        forward_v(last - 2)

        def block_step(i, _):
            h = last - i
            slot = h % 2
            vslot = h % 3

            @pl.when(jnp.logical_and(slot == 1, h < last))
            def _():
                collect_z((h - 1) // 2)

            @pl.when(h < last)
            def _():
                product(h, vslot, whole)

            @pl.when(gathered(h))
            def _():
                w_act1(1)
                w_act1(0)

            @pl.when(h != last - 1)
            def _():
                merge(h, slot)

            @pl.when(h == last - 1)
            def _():
                act_p2(slot)

            @pl.when(jnp.logical_and(h > 0, h < last))
            def _():
                act_rs2(1 - slot)
            for hh in range(blocks - AHEAD):
                @pl.when(h == hh + AHEAD)
                def _():
                    issue_v(hh)
            for hh in range(blocks - 2):
                @pl.when(h - 2 == hh)
                def _():
                    collect_v(hh)

            @pl.when(h > 1)
            def _():
                prepare(h - 2, (h - 2) % 3)
            for hh in range(blocks - 3):
                @pl.when(h - 3 == hh)
                def _():
                    v_loc(hh).start()

            @pl.when(h < GATHER)
            def _():
                act_w(1)

            @pl.when(gathered(h))
            def _():
                w_act2(1)
                w_act2(0)

            @pl.when(h > 1)
            def _():
                gram(h - 2, (h - 2) % 3)

            @pl.when(h < GATHER)
            def _():
                act_w(0)

            @pl.when(h == last - 1)
            def _():
                merge(h, slot)

            @pl.when(jnp.logical_and(h > 0, h < last))
            def _():
                act_ag2(1 - slot)

            @pl.when(h > 1)
            def _():
                send_g(slot)

            @pl.when(h == last)
            def _():
                for part in range(2):
                    issue_z(top - 2, part)

            @pl.when(jnp.logical_and(h <= last - 2, h >= last - top + 1))
            def _():
                for part in range(2):
                    issue_z(h - (last - top + 1), part)
            for hh in range(blocks - 3):
                @pl.when(h - 3 == hh)
                def _():
                    forward_v(hh)
            factor(slot)
            yb = dot(reduced(h, 1), nbuf[...], 1, 1)
            ws[1] = yb[:, 256:512]
            update(h, vslot, 1, yb[:, 0:256])
            ya = dot(reduced(h, 0), tbuf[slot, 0], 1, 1) - ws[1]
            update(h, vslot, 0, ya)

            @pl.when(jnp.logical_and(h > 0, h < last))
            def _():
                act_ag1(1 - slot)
            return 0

        lax.fori_loop(0, blocks, block_step, 0)
        stages = [buf.at[k] for buf in (wacc, r1, ws, r2) for k in range(2)]
        outs = []
        for t in range(rows // TILE):
            if t >= len(stages):
                outs[t - len(stages)].wait()
            stages[t % len(stages)][...] = xt[t].T
            outs.append(pltpu.make_async_copy(stages[t % len(stages)], o_hbm.at[pl.ds(TILE * t, TILE), :], o_s.at[t]))
            outs[t].start()
        for cp in outs[-len(stages):]:
            cp.wait()
        for hh in range(blocks):
            v_x(hh).wait_send()
            v_sib(hh).wait_send()
            v_fwd(hh).wait_send()
            for cp in t_copies(hh):
                cp.wait_send()
        for t in range(rows // TILE):
            for part in range(2):
                for cp in z_copies(t, part):
                    cp.wait_send()

    return body


def solution(mesh):
    def local(v_loc, t_loc, z_loc):
        rows, cols = v_loc.shape
        blocks = cols // 128
        t_loc = t_loc.reshape(blocks, 2, 64, 64)
        tiles = ((blocks + 1) // 2) * ((blocks + 2) // 2)
        dma = pltpu.SemaphoreType.DMA
        hbm = pl.BlockSpec(memory_space=pl.ANY)
        return pl.pallas_call(
            make_kernel(rows, blocks),
            out_shape=jax.ShapeDtypeStruct((rows, 256), F32),
            in_specs=[hbm] * 3,
            out_specs=hbm,
            scratch_shapes=[
                pltpu.VMEM((3 * TILE * tiles + 2 * rows, 128), F32),
                pltpu.VMEM((3, 3, rows, 512), BF16),
                pltpu.VMEM((4, blocks, 64, 64), F32),
                pltpu.VMEM((rows // TILE, 256, TILE), F32),
                pltpu.VMEM((2, 256, 256), F32), pltpu.VMEM((2, 256, 256), F32),
                pltpu.VMEM((2, 256, 256), F32), pltpu.VMEM((2, 256, 256), F32),
                pltpu.VMEM((3, 256, 256), BF16),
                pltpu.VMEM((384, 256), F32),
                pltpu.VMEM((2, 448, 128), F32), pltpu.VMEM((2, 448, 128), F32),
                pltpu.VMEM((2, 448, 128), F32), pltpu.VMEM((2, 448, 128), F32),
                pltpu.VMEM((2, 2, 256, 256), F32),
                pltpu.VMEM((2, 256, 256), F32),
                pltpu.VMEM((512, 256), F32),
                dma((blocks,)), dma((blocks,)), dma((blocks,)), dma((blocks,)), dma((3, blocks)),
                dma((blocks,)), dma((blocks,)), dma((blocks,)), dma((blocks,)), dma((4, blocks)),
                dma((3, rows // TILE, 2)), dma((rows // TILE, 2)), dma((4, rows // TILE, 2)),
                dma((2, 2)), dma((2, 2)), dma((2, 2)), dma((2, 2)),
                dma((4, 2, 2)), dma((4, 2, 2)), dma((4, 2, 2)), dma((4, 2, 2)),
                dma((2, 2)), dma((2, 2)), dma((rows // TILE,)),
            ],
            compiler_params=pltpu.CompilerParams(collective_id=0, has_side_effects=True,
                                                 vmem_limit_bytes=67043328),
        )(v_loc, t_loc, z_loc.T)

    return jax.shard_map(local, mesh=mesh,
                         in_specs=(P('row', 'col'), P('col', None, None), P(None, ('col', 'row'))),
                         out_specs=P('row', 'col'), check_vma=False)
```

```python
import jax
import jax.numpy as jnp
from jax import lax
from jax.experimental import pallas as pl
from jax.experimental.pallas import tpu as pltpu
from jax.sharding import PartitionSpec as P

F32 = jnp.float32
BF16 = jnp.bfloat16
MESH = pl.DeviceIdType.MESH
TILE = 256
LANE = 128
WIDE = 64
PAIR = range(2)
AHEAD = 8
GATHER = 8


def dot(a, b, ca, cb):
    return lax.dot_general(a, b, (((ca,), (cb,)), ((), ())), preferred_element_type=F32,
                           precision=lax.Precision.HIGHEST)


def split(a):
    a1 = a.astype(BF16)
    rest = a - a1.astype(F32)
    a2 = rest.astype(BF16)
    return a1, a2, (rest - a2.astype(F32)).astype(BF16)


def dot6(pairs, ca, cb):
    lhs, rhs = [], []
    for (a1, a2, a3), (b1, b2, b3) in pairs:
        lhs += [a3, a1, a2, a1, a2, a1]
        rhs += [b1, b3, b2, b2, b1, b1]
    return lax.dot_general(jnp.concatenate(lhs, ca), jnp.concatenate(rhs, cb), (((ca,), (cb,)), ((), ())),
                           preferred_element_type=F32)


def make_kernel(rows, blocks):
    def tiles_of(h):
        return (blocks + 1 - h) // 2

    def tiles_before(h):
        k = blocks - 1 - h
        return ((k + 1) // 2) * ((k + 2) // 2)

    area = TILE * tiles_before(-1)

    def body(v_hbm, t_hbm, z_hbm, o_hbm, vbuf, vp, tall, xt, wacc, r1, ws, r2, yp, gkk, gacc, gr1, gr2, gf, tbuf, gab,
             nbuf, vx_s, vsib_s, vfwd_s, vloc_s, v_r, tx_s, txc_s, tsib_s, tloc_s, t_r, z_s, zloc_s, z_r,
             p1_s, p1_r, p2_s, p2_r, g_s, g_r, w_s, w_r, d_s, d_r, o_s):
        r = lax.axis_index("row")
        c = lax.axis_index("col")
        core = c % 2
        cx, csib, cxc = (c + 2) % 4, c + 1 - 2 * core, 3 - c
        ry, rz, rd = r + 1 - 2 * (r % 2), (r + 2) % 4, 3 - r
        dev_x, dev_sib, dev_xc = (r, cx), (r, csib), (r, cxc)
        dev_y, dev_z, dev_d = (ry, c), (rz, c), (rd, c)

        last = blocks - 1

        def remote(src, dst, ss, rs, dev):
            return pltpu.make_async_remote_copy(src, dst, ss, rs, device_id=dev, device_id_type=MESH)

        barrier = pltpu.get_barrier_semaphore()
        for dev in (dev_x, dev_sib, dev_xc, dev_y, dev_z, dev_d):
            pl.semaphore_signal(barrier, 1, device_id=dev, device_id_type=MESH)
        pl.semaphore_wait(barrier, 6)

        def v_src(hh):
            n = LANE * (blocks - hh)
            return v_hbm.at[pl.ds(rows - n, n), pl.ds(hh * LANE, LANE)]

        def v_rows(base, hh):
            return vbuf.at[pl.ds(base + LANE * (hh % 2), LANE * (blocks - hh)), :]

        def v_dst(rel, hh):
            return v_rows(area * (rel - 1) + TILE * tiles_before(hh), hh)

        def v_x(hh):
            return remote(v_src(hh), v_dst(2, hh), vx_s.at[hh], v_r.at[1, hh], dev_x)

        def v_sib(hh):
            return remote(v_src(hh), v_dst(1, hh), vsib_s.at[hh], v_r.at[0, hh], dev_sib)

        def v_fwd(hh):
            return remote(v_dst(2, hh), v_dst(3, hh), vfwd_s.at[hh], v_r.at[2, hh], dev_sib)

        def v_loc(hh):
            return pltpu.make_async_copy(v_src(hh), v_rows(3 * area + rows * (hh % 2), hh), vloc_s.at[hh])

        def clear_v():
            for rel in range(3):
                for hh in range(1, blocks, 2):
                    vbuf[pl.ds(area * rel + TILE * tiles_before(hh), LANE), :] = jnp.zeros((LANE, LANE), F32)
            vbuf[pl.ds(3 * area + rows, LANE), :] = jnp.zeros((LANE, LANE), F32)

        def v_arrive(rel, hh):
            return remote(v_src(hh), v_dst(rel, hh), vx_s.at[hh], v_r.at[rel - 1, hh], dev_x)

        def t_copies(h):
            return (remote(t_hbm.at[h, core], tall.at[c, h], tx_s.at[h], t_r.at[c, h], dev_x),
                    remote(t_hbm.at[h, 1 - core], tall.at[c, h], txc_s.at[h], t_r.at[c, h], dev_xc),
                    remote(t_hbm.at[h, 1 - core], tall.at[c, h], tsib_s.at[h], t_r.at[c, h], dev_sib))

        def t_loc(h):
            return pltpu.make_async_copy(t_hbm.at[h, core], tall.at[c, h], tloc_s.at[h])

        def t_arrive(slot, h):
            return remote(t_hbm.at[h, core], tall.at[slot, h], tx_s.at[h], t_r.at[slot, h], dev_x)

        def issue_v(hh):
            v_x(hh).start()
            v_sib(hh).start()
            for cp in t_copies(hh):
                cp.start()
            t_loc(hh).start()

        def forward_v(hh):
            v_arrive(2, hh).wait_recv()
            v_fwd(hh).start()

        def collect_v(hh):
            v_loc(hh).wait()
            v_arrive(1, hh).wait_recv()
            v_arrive(3, hh).wait_recv()
            t_loc(hh).wait()
            for slot in (cx, csib, cxc):
                t_arrive(slot, hh).wait_recv()

        def z_src(to, t, part):
            return z_hbm.at[:, pl.ds(pl.multiple_of(rows * to + TILE * t + LANE * part, LANE), LANE)]

        def z_dst(src_r, t, part):
            return xt.at[t, pl.ds(pl.multiple_of(WIDE * src_r, WIDE), WIDE), pl.ds(LANE * part, LANE)]

        def z_copies(t, part):
            return [remote(z_src(dev[0], t, part), z_dst(r, t, part), z_s.at[i, t, part], z_r.at[r, t, part], dev)
                    for i, dev in enumerate((dev_y, dev_z, dev_d))]

        def z_loc(t, part):
            return pltpu.make_async_copy(z_src(r, t, part), z_dst(r, t, part), zloc_s.at[t, part])

        def issue_z(t, part):
            for cp in z_copies(t, part):
                cp.start()
            z_loc(t, part).start()

        def collect_z(t):
            for part in PAIR:
                z_loc(t, part).wait()
                for src_r in (ry, rz, rd):
                    dst = z_dst(src_r, t, part)
                    remote(z_src(r, t, part), dst, z_s.at[0, t, part], z_r.at[src_r, t, part], dev_y).wait_recv()

        def steps(half):
            return (dev_y, dev_z) if half == 0 else (dev_z, dev_y)

        def w_p1(p, half):
            s = pl.ds(LANE * half, LANE)
            return remote(wacc.at[p, s], r1.at[p, s], p1_s.at[p, half], p1_r.at[p, half], steps(half)[0])

        def w_p2(p, half):
            s = pl.ds(LANE * half, LANE)
            return remote(ws.at[p, s], r2.at[p, s], p2_s.at[p, half], p2_r.at[p, half], steps(half)[1])

        def g_place(f):
            k1, k2 = ((r % 2), (r // 2)) if f == 0 else ((r // 2), (r % 2))
            return 224 * f, k1, k2

        def g_rows(start, n):
            return pl.ds(pl.multiple_of(start, 8), n)

        def w_kept(f, other=0):
            k1 = r % 2 if f == 0 else r // 2
            return g_rows(LANE * f + WIDE * (k1 + other * (1 - 2 * k1)), WIDE)

        def w_e1(p, f):
            s = w_kept(f, 1)
            return remote(wacc.at[p, s], r1.at[p, s], w_s.at[0, p, f], w_r.at[0, p, f], steps(f)[0])

        def w_e2(p, f):
            s = w_kept(f)
            return remote(ws.at[p, s], r2.at[p, s], w_s.at[1, p, f], w_r.at[1, p, f], steps(f)[1])

        def w_e3(p, f):
            s = w_kept(f)
            return remote(wacc.at[p, s], wacc.at[p, s], w_s.at[2, p, f], w_r.at[2, p, f], steps(f)[0])

        def w_act1(p):
            for f in PAIR:
                w_e1(p, f).wait()
            for f in PAIR:
                s = w_kept(f)
                ws[p, s] = wacc[p, s] + r1[p, s]
                w_e2(p, f).start()

        def w_act2(p):
            for f in PAIR:
                w_e2(p, f).wait()
            for f in PAIR:
                s = w_kept(f)
                wacc[p, s] = ws[p, s] + r2[p, s]
                w_e3(p, f).start()

        def g_p1(par, f):
            s = pl.ds(224 * f, 224)
            return remote(gacc.at[par, s], gr1.at[par, s], g_s.at[0, par, f], g_r.at[0, par, f], steps(f)[0])

        def g_p2(par, f):
            s = pl.ds(224 * f, 224)
            return remote(gacc.at[par, s], gr2.at[par, s], g_s.at[1, par, f], g_r.at[1, par, f], steps(f)[1])

        def act_p2(par):
            for f in PAIR:
                g_p1(par, f).wait()
            gacc[par] = gacc[par] + gr1[par]
            for f in PAIR:
                g_p2(par, f).start()

        def g_rs1(par, f):
            base, k1, _ = g_place(f)
            s = g_rows(base + 112 * (1 - k1), 112)
            return remote(gacc.at[par, s], gr1.at[par, s], g_s.at[0, par, f], g_r.at[0, par, f], steps(f)[0])

        def g_rs2(par, f):
            base, k1, k2 = g_place(f)
            s = g_rows(base + 112 * k1 + 56 * (1 - k2), 56)
            return remote(gacc.at[par, s], gr2.at[par, s], g_s.at[1, par, f], g_r.at[1, par, f], steps(f)[1])

        def g_ag2(par, f):
            base, k1, k2 = g_place(f)
            s = g_rows(base + 112 * k1 + 56 * k2, 56)
            return remote(gf.at[par, s], gf.at[par, s], g_s.at[2, par, f], g_r.at[2, par, f], steps(f)[1])

        def g_ag1(par, f):
            base, k1, _ = g_place(f)
            s = g_rows(base + 112 * k1, 112)
            return remote(gf.at[par, s], gf.at[par, s], g_s.at[3, par, f], g_r.at[3, par, f], steps(f)[0])

        def act_rs2(par):
            for f in PAIR:
                g_rs1(par, f).wait()
            for f in PAIR:
                base, k1, _ = g_place(f)
                s = g_rows(base + 112 * k1, 112)
                gacc[par, s] = gacc[par, s] + gr1[par, s]
                g_rs2(par, f).start()

        def act_ag2(par):
            for f in PAIR:
                base, k1, k2 = g_place(f)
                g_rs2(par, f).wait()
                s = g_rows(base + 112 * k1 + 56 * k2, 56)
                gf[par, s] = gacc[par, s] + gr2[par, s]
                g_ag2(par, f).start()

        def act_ag1(par):
            for f in PAIR:
                g_ag2(par, f).wait()
                g_ag1(par, f).start()

        def over_tiles(n, fn):
            def four(t, _):
                fn(4 * t, 4)
                return 0
            lax.fori_loop(0, n // 4, four, 0)

            @pl.when(n % 4 >= 2)
            def _():
                fn(4 * (n // 4), 2)

            @pl.when(n % 2 == 1)
            def _():
                fn(n - 1, 1)

        def whole(n, fn):
            for k in range(1, rows // TILE + 1):
                @pl.when(n == k)
                def _():
                    fn(0, k)

        def prepare(h, slot):
            bases = []
            for i in range(4):
                rel = ((c // 2 + i // 2) % 2) * 2 + (c + i) % 2
                own = (3 - rel) // 3
                bases.append(own * (3 * area + rows * (h % 2)) + (1 - own) * (area * (rel - 1) + TILE * tiles_before(h)))

            def one(t, _):
                d = pl.ds(pl.multiple_of(TILE * t, TILE), TILE)
                for i in PAIR:
                    a = vbuf[pl.ds(pl.multiple_of(bases[2 * i] + TILE * t, TILE), TILE), :]
                    b = vbuf[pl.ds(pl.multiple_of(bases[2 * i + 1] + TILE * t, TILE), TILE), :]
                    low = lax.broadcasted_iota(jnp.int32, a.shape, 1) < WIDE
                    ar, br = pltpu.roll(a, WIDE, 1), pltpu.roll(b, WIDE, 1)
                    for k, part in enumerate(split(jnp.where(low, a, br))):
                        vp[slot, k, d, LANE * i:LANE * i + LANE] = part
                    for k, part in enumerate(split(jnp.where(low, ar, b))):
                        vp[slot, k, d, TILE + LANE * i:TILE + LANE * i + LANE] = part
                return 0
            lax.fori_loop(0, tiles_of(h), one, 0)

        def parts(slot, t, lanes):
            s = pl.ds(pl.multiple_of(TILE * t, TILE), TILE)
            return tuple(vp[slot, k, s, lanes] for k in range(3))

        def gram(h, slot):
            gkk[...] = jnp.zeros_like(gkk)
            mine = pl.ds(pl.multiple_of(TILE * core, TILE), TILE)
            half = pl.ds(pl.multiple_of(LANE * core, LANE), LANE)

            def one(t, n):
                own = [parts(slot, t + u, mine) for u in range(n)]
                gkk[0:TILE, :] += dot6([(a, a) for a in own], 0, 0)
                gkk[TILE:384, :] += dot6([(parts(slot, t + u, half), parts(slot, t + u, pl.ds(TILE, TILE)))
                                         for u in range(n)], 0, 0)
            over_tiles(tiles_of(h), one)

        def send_g(par, first=g_rs1):
            gacc[par, 0:LANE, :] = gkk[TILE:384, 0:LANE]
            gacc[par, LANE:TILE, :] = gkk[TILE:384, LANE:TILE]
            gacc[par, TILE:384, :] = gkk[0:LANE, LANE:TILE]
            gacc[par, 384:448, 0:WIDE] = gkk[0:WIDE, WIDE:LANE]
            gacc[par, 384:448, WIDE:LANE] = gkk[LANE:192, 192:TILE]
            for f in PAIR:
                first(par, f).start()

        def rows_of(k):
            return pl.ds(pl.multiple_of(LANE * k, LANE), LANE)

        def share(slot, k):
            return (remote(tbuf.at[slot, k], tbuf.at[slot, k], d_s.at[slot, 0], d_r.at[slot, 0], dev_sib),
                    remote(gab.at[slot, rows_of(k)], gab.at[slot, rows_of(k)], d_s.at[slot, 1], d_r.at[slot, 1], dev_sib))

        def merge(h, slot):
            @pl.when(h >= last - 1)
            def _():
                for f in PAIR:
                    g_p2(slot, f).wait()
                gf[slot] = gacc[slot] + gr2[slot]

            @pl.when(h < last - 1)
            def _():
                for f in PAIR:
                    g_ag1(slot, f).wait()
            g = gf[slot]
            gab[slot, rows_of(core), 0:LANE] = g[0:LANE]
            gab[slot, rows_of(core), LANE:TILE] = g[LANE:TILE]
            zero = jnp.zeros((WIDE, WIDE), F32)

            def diag(a, b):
                return jnp.concatenate([jnp.concatenate([a, zero], 1), jnp.concatenate([zero, b], 1)], 0)
            t0, t1, t2, t3 = (tall[i, h] for i in range(4))
            low = g[384:448]
            off = dot(diag(low[:, 0:WIDE], low[:, WIDE:LANE]), diag(t1, t3), 1, 0)
            off = -dot(diag(t0, t2), off, 1, 0)
            ta = jnp.concatenate([jnp.concatenate([t0, off[0:WIDE, 0:WIDE]], 1), jnp.concatenate([zero, t1], 1)], 0)
            tb = jnp.concatenate([jnp.concatenate([t2, off[WIDE:LANE, WIDE:LANE]], 1), jnp.concatenate([zero, t3], 1)], 0)
            cross = -dot(ta, dot(g[TILE:384], tb, 1, 0), 1, 0)
            tbuf[slot, core, 0:LANE, 0:LANE] = ta
            tbuf[slot, core, 0:LANE, LANE:TILE] = cross
            tbuf[slot, core, LANE:TILE, 0:LANE] = jnp.zeros((LANE, LANE), F32)
            tbuf[slot, core, LANE:TILE, LANE:TILE] = tb
            for cp in share(slot, core):
                cp.start()

        def factor(slot):
            for cp in share(slot, core):
                cp.wait_send()
            for cp in share(slot, 1 - core):
                cp.wait_recv()
            tb = tbuf[slot, 1]
            nbuf[0:TILE, :] = tb
            nbuf[TILE:512, :] = dot(dot(tbuf[slot, 0], gab[slot], 1, 0), tb, 1, 0)

        def gathered(h):
            return jnp.logical_and(h >= GATHER, h < last)

        def pairwise(h):
            return jnp.logical_or(h < GATHER, h == last)

        def product(h, slot, run):
            t0 = rows // TILE - tiles_of(h)

            def group(i, _):
                p = 1 - i
                wacc[p] = jnp.zeros((TILE, TILE), F32)
                lanes = pl.ds(pl.multiple_of(TILE * p, TILE), TILE)

                def one(t, n):
                    wacc[p] += dot6([(split(xt[t0 + t + u]), parts(slot, t + u, lanes)) for u in range(n)], 1, 0)
                run(tiles_of(h), one)
                if run is whole:
                    @pl.when(gathered(h))
                    def _():
                        for f in PAIR:
                            w_e1(p, f).start()

                    @pl.when(h < GATHER)
                    def _():
                        for half in PAIR:
                            w_p1(p, half).start()
                else:
                    for half in PAIR:
                        w_p1(p, half).start()
                return 0
            lax.fori_loop(0, 2, group, 0)

        def act_w(p):
            for half in PAIR:
                w_p1(p, half).wait()
            ws[p] = wacc[p] + r1[p]
            for half in PAIR:
                w_p2(p, half).start()

        def reduced(h, p):
            @pl.when(gathered(h))
            def _():
                for f in PAIR:
                    w_e3(p, f).wait()

            @pl.when(pairwise(h))
            def _():
                for half in PAIR:
                    w_p2(p, half).wait()
                wacc[p] = ws[p] + r2[p]
            return wacc[p]

        def update(h, slot, p, y):
            for k, part in enumerate(split(-y)):
                yp[k] = part
            t0 = rows // TILE - tiles_of(h)

            def one(t, n):
                for u in range(n):
                    xt[t0 + t + u] += dot6([(tuple(yp[k] for k in range(3)), parts(slot, t + u, pl.ds(TILE * p, TILE)))], 1, 1)
            whole(tiles_of(h), one)

        def ready(h, slot):
            collect_v(h)
            prepare(h, slot)
            gram(h, slot)

        def ready(h, slot):
            collect_v(h)
            prepare(h, slot)
            gram(h, slot)

        top = rows // TILE - 1
        issue_v(last)
        v_loc(last).start()
        for part in PAIR:
            issue_z(top, part)
        for hh in range(last - 1, last - AHEAD, -1):
            issue_v(hh)
        v_loc(last - 1).start()
        for part in PAIR:
            issue_z(top - 1, part)
        clear_v()
        forward_v(last)
        ready(last, last % 3)
        send_g(last % 2, g_p1)
        collect_z(top)
        product(last, last % 3, lambda n, fn: fn(0, 1))
        forward_v(last - 1)
        v_loc(last - 2).start()
        ready(last - 1, (last - 1) % 3)
        act_p2(last % 2)
        act_w(1)
        act_w(0)
        send_g((last - 1) % 2, g_p1)
        forward_v(last - 2)

        def block_step(i, _):
            h = last - i
            slot = h % 2
            vslot = h % 3

            @pl.when(jnp.logical_and(slot == 1, h < last))
            def _():
                collect_z((h - 1) // 2)

            @pl.when(h < last)
            def _():
                product(h, vslot, whole)

            @pl.when(gathered(h))
            def _():
                w_act1(1)
                w_act1(0)

            @pl.when(h != last - 1)
            def _():
                merge(h, slot)

            @pl.when(h == last - 1)
            def _():
                act_p2(slot)

            @pl.when(jnp.logical_and(h > 0, h < last))
            def _():
                act_rs2(1 - slot)
            for hh in range(blocks - AHEAD):
                @pl.when(h == hh + AHEAD)
                def _():
                    issue_v(hh)
            for hh in range(blocks - 2):
                @pl.when(h - 2 == hh)
                def _():
                    collect_v(hh)

            @pl.when(h > 1)
            def _():
                prepare(h - 2, (h - 2) % 3)
            for hh in range(blocks - 3):
                @pl.when(h - 3 == hh)
                def _():
                    v_loc(hh).start()

            @pl.when(h < GATHER)
            def _():
                act_w(1)

            @pl.when(gathered(h))
            def _():
                w_act2(1)
                w_act2(0)

            @pl.when(h > 1)
            def _():
                gram(h - 2, (h - 2) % 3)

            @pl.when(h < GATHER)
            def _():
                act_w(0)

            @pl.when(h == last - 1)
            def _():
                merge(h, slot)

            @pl.when(jnp.logical_and(h > 0, h < last))
            def _():
                act_ag2(1 - slot)

            @pl.when(h > 1)
            def _():
                send_g(slot)

            @pl.when(jnp.logical_and(h < last, h >= last - top + 1))
            def _():
                for part in PAIR:
                    issue_z(h - (last - top + 1), part)
            for hh in range(blocks - 3):
                @pl.when(h - 3 == hh)
                def _():
                    forward_v(hh)
            factor(slot)
            yb = dot(reduced(h, 1), nbuf[...], 1, 1)
            ws[1] = yb[:, TILE:512]
            update(h, vslot, 1, yb[:, 0:TILE])
            ya = dot(reduced(h, 0), tbuf[slot, 0], 1, 1) - ws[1]
            update(h, vslot, 0, ya)

            @pl.when(jnp.logical_and(h > 0, h < last))
            def _():
                act_ag1(1 - slot)
            return 0

        lax.fori_loop(0, blocks, block_step, 0)
        out = pltpu.make_async_copy(xt, o_hbm, o_s)
        out.start()
        for hh in range(blocks):
            v_x(hh).wait_send()
            v_sib(hh).wait_send()
            v_fwd(hh).wait_send()
            for cp in t_copies(hh):
                cp.wait_send()
        for t in range(rows // TILE):
            for part in PAIR:
                for cp in z_copies(t, part):
                    cp.wait_send()
        out.wait()

    return body


def solution(mesh):
    def local(v_loc, t_loc, z_loc):
        rows, cols = v_loc.shape
        blocks = cols // LANE
        t_loc = t_loc.reshape(blocks, 2, WIDE, WIDE)
        tiles = ((blocks + 1) // 2) * ((blocks + 2) // 2)
        dma = pltpu.SemaphoreType.DMA
        hbm = pl.BlockSpec(memory_space=pl.ANY)
        xt = pl.pallas_call(
            make_kernel(rows, blocks),
            out_shape=jax.ShapeDtypeStruct((rows // TILE, TILE, TILE), F32),
            in_specs=[hbm] * 3,
            out_specs=hbm,
            scratch_shapes=[
                pltpu.VMEM((3 * TILE * tiles + 2 * rows, LANE), F32),
                pltpu.VMEM((3, 3, rows, 512), BF16),
                pltpu.VMEM((4, blocks, WIDE, WIDE), F32),
                pltpu.VMEM((rows // TILE, TILE, TILE), F32),
                pltpu.VMEM((2, TILE, TILE), F32), pltpu.VMEM((2, TILE, TILE), F32),
                pltpu.VMEM((2, TILE, TILE), F32), pltpu.VMEM((2, TILE, TILE), F32),
                pltpu.VMEM((3, TILE, TILE), BF16),
                pltpu.VMEM((384, TILE), F32),
                pltpu.VMEM((2, 448, LANE), F32), pltpu.VMEM((2, 448, LANE), F32),
                pltpu.VMEM((2, 448, LANE), F32), pltpu.VMEM((2, 448, LANE), F32),
                pltpu.VMEM((2, 2, TILE, TILE), F32),
                pltpu.VMEM((2, TILE, TILE), F32),
                pltpu.VMEM((512, TILE), F32),
                dma((blocks,)), dma((blocks,)), dma((blocks,)), dma((blocks,)), dma((3, blocks)),
                dma((blocks,)), dma((blocks,)), dma((blocks,)), dma((blocks,)), dma((4, blocks)),
                dma((3, rows // TILE, 2)), dma((rows // TILE, 2)), dma((4, rows // TILE, 2)),
                dma((2, 2)), dma((2, 2)), dma((2, 2)), dma((2, 2)),
                dma((4, 2, 2)), dma((4, 2, 2)), dma((4, 2, 2)), dma((4, 2, 2)),
                dma((2, 2)), dma((2, 2)), dma,
            ],
            compiler_params=pltpu.CompilerParams(collective_id=0, has_side_effects=True,
                                                 vmem_limit_bytes=67043328),
        )(v_loc, t_loc, z_loc.T)

        return xt.transpose(0, 2, 1).reshape(rows, TILE)

    return jax.shard_map(local, mesh=mesh,
                         in_specs=(P('row', 'col'), P('col', None, None), P(None, ('col', 'row'))),
                         out_specs=P('row', 'col'), check_vma=False)
```

```python
import jax
import jax.numpy as jnp
from jax import lax
from jax.experimental import pallas as pl
from jax.experimental.pallas import tpu as pltpu
from jax.sharding import PartitionSpec as P

F32 = jnp.float32
BF16 = jnp.bfloat16
MESH = pl.DeviceIdType.MESH
TILE = 256
LANE = 128
WIDE = 64
PAIR = range(2)
AHEAD = 8
GATHER = 8
EARLY = 4


def dot(a, b, ca, cb):
    return lax.dot_general(a, b, (((ca,), (cb,)), ((), ())), preferred_element_type=F32,
                           precision=lax.Precision.HIGHEST)


def split(a):
    a1 = a.astype(BF16)
    rest = a - a1.astype(F32)
    a2 = rest.astype(BF16)
    return a1, a2, (rest - a2.astype(F32)).astype(BF16)


def dot6(pairs, ca, cb):
    lhs, rhs = [], []
    for (a1, a2, a3), (b1, b2, b3) in pairs:
        lhs += [a3, a1, a2, a1, a2, a1]
        rhs += [b1, b3, b2, b2, b1, b1]
    return lax.dot_general(jnp.concatenate(lhs, ca), jnp.concatenate(rhs, cb), (((ca,), (cb,)), ((), ())),
                           preferred_element_type=F32)


def make_kernel(rows, blocks):
    def tiles_of(h):
        return (blocks + 1 - h) // 2

    def tiles_before(h):
        k = blocks - 1 - h
        return ((k + 1) // 2) * ((k + 2) // 2)

    area = TILE * tiles_before(-1)

    def body(v_hbm, t_hbm, z_hbm, o_hbm, vbuf, vp, tall, xt, wacc, r1, ws, r2, yp, gkk, gacc, gr1, gr2, gf, tbuf, gab,
             nbuf, vx_s, vsib_s, vfwd_s, vloc_s, v_r, tx_s, txc_s, tsib_s, tloc_s, t_r, z_s, zloc_s, z_r,
             p1_s, p1_r, p2_s, p2_r, g_s, g_r, w_s, w_r, d_s, d_r, o_s):
        r = lax.axis_index("row")
        c = lax.axis_index("col")
        core = c % 2
        cx, csib, cxc = (c + 2) % 4, c + 1 - 2 * core, 3 - c
        ry, rz, rd = r + 1 - 2 * (r % 2), (r + 2) % 4, 3 - r
        dev_x, dev_sib, dev_xc = (r, cx), (r, csib), (r, cxc)
        dev_y, dev_z, dev_d = (ry, c), (rz, c), (rd, c)

        last = blocks - 1

        def remote(src, dst, ss, rs, dev):
            return pltpu.make_async_remote_copy(src, dst, ss, rs, device_id=dev, device_id_type=MESH)

        barrier = pltpu.get_barrier_semaphore()
        for dev in (dev_x, dev_sib, dev_xc, dev_y, dev_z, dev_d):
            pl.semaphore_signal(barrier, 1, device_id=dev, device_id_type=MESH)
        pl.semaphore_wait(barrier, 6)

        def v_src(hh):
            n = LANE * (blocks - hh)
            return v_hbm.at[pl.ds(rows - n, n), pl.ds(hh * LANE, LANE)]

        def v_rows(base, hh):
            return vbuf.at[pl.ds(base + LANE * (hh % 2), LANE * (blocks - hh)), :]

        def v_dst(rel, hh):
            return v_rows(area * (rel - 1) + TILE * tiles_before(hh), hh)

        def v_x(hh):
            return remote(v_src(hh), v_dst(2, hh), vx_s.at[hh], v_r.at[1, hh], dev_x)

        def v_sib(hh):
            return remote(v_src(hh), v_dst(1, hh), vsib_s.at[hh], v_r.at[0, hh], dev_sib)

        def v_fwd(hh):
            return remote(v_dst(2, hh), v_dst(3, hh), vfwd_s.at[hh], v_r.at[2, hh], dev_sib)

        def v_loc(hh):
            return pltpu.make_async_copy(v_src(hh), v_rows(3 * area + rows * (hh % 2), hh), vloc_s.at[hh])

        def clear_v():
            for rel in range(3):
                for hh in range(1, blocks, 2):
                    vbuf[pl.ds(area * rel + TILE * tiles_before(hh), LANE), :] = jnp.zeros((LANE, LANE), F32)
            vbuf[pl.ds(3 * area + rows, LANE), :] = jnp.zeros((LANE, LANE), F32)

        def v_arrive(rel, hh):
            return remote(v_src(hh), v_dst(rel, hh), vx_s.at[hh], v_r.at[rel - 1, hh], dev_x)

        def t_copies(h):
            return (remote(t_hbm.at[h, core], tall.at[c, h], tx_s.at[h], t_r.at[c, h], dev_x),
                    remote(t_hbm.at[h, 1 - core], tall.at[c, h], txc_s.at[h], t_r.at[c, h], dev_xc),
                    remote(t_hbm.at[h, 1 - core], tall.at[c, h], tsib_s.at[h], t_r.at[c, h], dev_sib))

        def t_loc(h):
            return pltpu.make_async_copy(t_hbm.at[h, core], tall.at[c, h], tloc_s.at[h])

        def t_arrive(slot, h):
            return remote(t_hbm.at[h, core], tall.at[slot, h], tx_s.at[h], t_r.at[slot, h], dev_x)

        def issue_v(hh):
            v_x(hh).start()
            v_sib(hh).start()
            for cp in t_copies(hh):
                cp.start()
            t_loc(hh).start()

        def forward_v(hh):
            v_arrive(2, hh).wait_recv()
            v_fwd(hh).start()

        def collect_v(hh):
            v_loc(hh).wait()
            v_arrive(1, hh).wait_recv()
            v_arrive(3, hh).wait_recv()
            t_loc(hh).wait()
            for slot in (cx, csib, cxc):
                t_arrive(slot, hh).wait_recv()

        def z_src(to, t, part):
            return z_hbm.at[:, pl.ds(pl.multiple_of(rows * to + TILE * t + LANE * part, LANE), LANE)]

        def z_dst(src_r, t, part):
            return xt.at[t, pl.ds(pl.multiple_of(WIDE * src_r, WIDE), WIDE), pl.ds(LANE * part, LANE)]

        def z_copies(t, part):
            return [remote(z_src(dev[0], t, part), z_dst(r, t, part), z_s.at[i, t, part], z_r.at[r, t, part], dev)
                    for i, dev in enumerate((dev_y, dev_z, dev_d))]

        def z_loc(t, part):
            return pltpu.make_async_copy(z_src(r, t, part), z_dst(r, t, part), zloc_s.at[t, part])

        def issue_z(t, part):
            for cp in z_copies(t, part):
                cp.start()
            z_loc(t, part).start()

        def collect_z(t):
            for part in PAIR:
                z_loc(t, part).wait()
                for src_r in (ry, rz, rd):
                    dst = z_dst(src_r, t, part)
                    remote(z_src(r, t, part), dst, z_s.at[0, t, part], z_r.at[src_r, t, part], dev_y).wait_recv()

        def steps(half):
            return (dev_y, dev_z) if half == 0 else (dev_z, dev_y)

        def w_p1(p, half):
            s = pl.ds(LANE * half, LANE)
            return remote(wacc.at[p, s], r1.at[p, s], p1_s.at[p, half], p1_r.at[p, half], steps(half)[0])

        def w_p2(p, half):
            s = pl.ds(LANE * half, LANE)
            return remote(ws.at[p, s], r2.at[p, s], p2_s.at[p, half], p2_r.at[p, half], steps(half)[1])

        def g_place(f):
            k1, k2 = ((r % 2), (r // 2)) if f == 0 else ((r // 2), (r % 2))
            return 224 * f, k1, k2

        def g_rows(start, n):
            return pl.ds(pl.multiple_of(start, 8), n)

        def w_kept(f, other=0):
            k1 = r % 2 if f == 0 else r // 2
            return g_rows(LANE * f + WIDE * (k1 + other * (1 - 2 * k1)), WIDE)

        def w_e1(p, f):
            s = w_kept(f, 1)
            return remote(wacc.at[p, s], r1.at[p, s], w_s.at[0, p, f], w_r.at[0, p, f], steps(f)[0])

        def w_e2(p, f):
            s = w_kept(f)
            return remote(ws.at[p, s], r2.at[p, s], w_s.at[1, p, f], w_r.at[1, p, f], steps(f)[1])

        def w_e3(p, f):
            s = w_kept(f)
            return remote(wacc.at[p, s], wacc.at[p, s], w_s.at[2, p, f], w_r.at[2, p, f], steps(f)[0])

        def w_act1(p):
            for f in PAIR:
                w_e1(p, f).wait()
            for f in PAIR:
                s = w_kept(f)
                ws[p, s] = wacc[p, s] + r1[p, s]
                w_e2(p, f).start()

        def w_act2(p):
            for f in PAIR:
                w_e2(p, f).wait()
            for f in PAIR:
                s = w_kept(f)
                wacc[p, s] = ws[p, s] + r2[p, s]
                w_e3(p, f).start()

        def g_p1(par, f):
            s = pl.ds(224 * f, 224)
            return remote(gacc.at[par, s], gr1.at[par, s], g_s.at[0, par, f], g_r.at[0, par, f], steps(f)[0])

        def g_p2(par, f):
            s = pl.ds(224 * f, 224)
            return remote(gacc.at[par, s], gr2.at[par, s], g_s.at[1, par, f], g_r.at[1, par, f], steps(f)[1])

        def act_p2(par):
            for f in PAIR:
                g_p1(par, f).wait()
            gacc[par] = gacc[par] + gr1[par]
            for f in PAIR:
                g_p2(par, f).start()

        def g_rs1(par, f):
            base, k1, _ = g_place(f)
            s = g_rows(base + 112 * (1 - k1), 112)
            return remote(gacc.at[par, s], gr1.at[par, s], g_s.at[0, par, f], g_r.at[0, par, f], steps(f)[0])

        def g_rs2(par, f):
            base, k1, k2 = g_place(f)
            s = g_rows(base + 112 * k1 + 56 * (1 - k2), 56)
            return remote(gacc.at[par, s], gr2.at[par, s], g_s.at[1, par, f], g_r.at[1, par, f], steps(f)[1])

        def g_ag2(par, f):
            base, k1, k2 = g_place(f)
            s = g_rows(base + 112 * k1 + 56 * k2, 56)
            return remote(gf.at[par, s], gf.at[par, s], g_s.at[2, par, f], g_r.at[2, par, f], steps(f)[1])

        def g_ag1(par, f):
            base, k1, _ = g_place(f)
            s = g_rows(base + 112 * k1, 112)
            return remote(gf.at[par, s], gf.at[par, s], g_s.at[3, par, f], g_r.at[3, par, f], steps(f)[0])

        def act_rs2(par):
            for f in PAIR:
                g_rs1(par, f).wait()
            for f in PAIR:
                base, k1, _ = g_place(f)
                s = g_rows(base + 112 * k1, 112)
                gacc[par, s] = gacc[par, s] + gr1[par, s]
                g_rs2(par, f).start()

        def act_ag2(par):
            for f in PAIR:
                base, k1, k2 = g_place(f)
                g_rs2(par, f).wait()
                s = g_rows(base + 112 * k1 + 56 * k2, 56)
                gf[par, s] = gacc[par, s] + gr2[par, s]
                g_ag2(par, f).start()

        def act_ag1(par):
            for f in PAIR:
                g_ag2(par, f).wait()
                g_ag1(par, f).start()

        def over_tiles(n, fn):
            def four(t, _):
                fn(4 * t, 4)
                return 0
            lax.fori_loop(0, n // 4, four, 0)

            @pl.when(n % 4 >= 2)
            def _():
                fn(4 * (n // 4), 2)

            @pl.when(n % 2 == 1)
            def _():
                fn(n - 1, 1)

        def whole(n, fn):
            for k in range(1, rows // TILE + 1):
                @pl.when(n == k)
                def _():
                    fn(0, k)

        def prepare(h, slot, start, stop):
            bases = []
            for i in range(4):
                rel = ((c // 2 + i // 2) % 2) * 2 + (c + i) % 2
                own = (3 - rel) // 3
                bases.append(own * (3 * area + rows * (h % 2)) + (1 - own) * (area * (rel - 1) + TILE * tiles_before(h)))

            def one(t, _):
                d = pl.ds(pl.multiple_of(TILE * t, TILE), TILE)
                for i in PAIR:
                    a = vbuf[pl.ds(pl.multiple_of(bases[2 * i] + TILE * t, TILE), TILE), :]
                    b = vbuf[pl.ds(pl.multiple_of(bases[2 * i + 1] + TILE * t, TILE), TILE), :]
                    low = lax.broadcasted_iota(jnp.int32, a.shape, 1) < WIDE
                    ar, br = pltpu.roll(a, WIDE, 1), pltpu.roll(b, WIDE, 1)
                    for k, part in enumerate(split(jnp.where(low, a, br))):
                        vp[slot, k, d, LANE * i:LANE * i + LANE] = part
                    for k, part in enumerate(split(jnp.where(low, ar, b))):
                        vp[slot, k, d, TILE + LANE * i:TILE + LANE * i + LANE] = part
                return 0
            lax.fori_loop(start, stop, one, 0)

        def parts(slot, t, lanes):
            s = pl.ds(pl.multiple_of(TILE * t, TILE), TILE)
            return tuple(vp[slot, k, s, lanes] for k in range(3))

        top3 = LANE + WIDE

        def gram_own(h, slot):
            gkk[0:top3, :] = jnp.zeros((top3, TILE), F32)
            mine = pl.ds(pl.multiple_of(TILE * core, TILE), TILE)

            def one(t, n):
                own = [parts(slot, t + u, mine) for u in range(n)]
                gkk[0:top3, :] += dot6([(tuple(x[:, 0:top3] for x in a), a) for a in own], 0, 0)
            over_tiles(tiles_of(h), one)

        def gram_cross(h, slot):
            gkk[TILE:TILE + LANE, :] = jnp.zeros((LANE, TILE), F32)
            half = pl.ds(pl.multiple_of(LANE * core, LANE), LANE)

            def one(t, n):
                gkk[TILE:TILE + LANE, :] += dot6([(parts(slot, t + u, half), parts(slot, t + u, pl.ds(TILE, TILE)))
                                                  for u in range(n)], 0, 0)
            over_tiles(tiles_of(h), one)

        def send_g(par, first=g_rs1):
            gacc[par, 0:LANE, :] = gkk[TILE:384, 0:LANE]
            gacc[par, LANE:TILE, :] = gkk[TILE:384, LANE:TILE]
            gacc[par, TILE:384, :] = gkk[0:LANE, LANE:TILE]
            gacc[par, 384:448, 0:WIDE] = gkk[0:WIDE, WIDE:LANE]
            gacc[par, 384:448, WIDE:LANE] = gkk[LANE:192, 192:TILE]
            for f in PAIR:
                first(par, f).start()

        def rows_of(k):
            return pl.ds(pl.multiple_of(LANE * k, LANE), LANE)

        def share(slot, k):
            return (remote(tbuf.at[slot, k], tbuf.at[slot, k], d_s.at[slot, 0], d_r.at[slot, 0], dev_sib),
                    remote(gab.at[slot, rows_of(k)], gab.at[slot, rows_of(k)], d_s.at[slot, 1], d_r.at[slot, 1], dev_sib))

        def merge(h, slot):
            @pl.when(jnp.logical_or(h >= last - 1, h == 0))
            def _():
                for f in PAIR:
                    g_p2(slot, f).wait()
                gf[slot] = gacc[slot] + gr2[slot]

            @pl.when(jnp.logical_and(h > 0, h < last - 1))
            def _():
                for f in PAIR:
                    g_ag1(slot, f).wait()
            g = gf[slot]
            gab[slot, rows_of(core), 0:LANE] = g[0:LANE]
            gab[slot, rows_of(core), LANE:TILE] = g[LANE:TILE]
            zero = jnp.zeros((WIDE, WIDE), F32)

            def diag(a, b):
                return jnp.concatenate([jnp.concatenate([a, zero], 1), jnp.concatenate([zero, b], 1)], 0)
            t0, t1, t2, t3 = (tall[i, h] for i in range(4))
            low = g[384:448]
            off = dot(diag(low[:, 0:WIDE], low[:, WIDE:LANE]), diag(t1, t3), 1, 0)
            off = -dot(diag(t0, t2), off, 1, 0)
            ta = jnp.concatenate([jnp.concatenate([t0, off[0:WIDE, 0:WIDE]], 1), jnp.concatenate([zero, t1], 1)], 0)
            tb = jnp.concatenate([jnp.concatenate([t2, off[WIDE:LANE, WIDE:LANE]], 1), jnp.concatenate([zero, t3], 1)], 0)
            cross = -dot(ta, dot(g[TILE:384], tb, 1, 0), 1, 0)
            tbuf[slot, core, 0:LANE, 0:LANE] = ta
            tbuf[slot, core, 0:LANE, LANE:TILE] = cross
            tbuf[slot, core, LANE:TILE, 0:LANE] = jnp.zeros((LANE, LANE), F32)
            tbuf[slot, core, LANE:TILE, LANE:TILE] = tb
            for cp in share(slot, core):
                cp.start()

        def factor(slot):
            for cp in share(slot, core):
                cp.wait_send()
            for cp in share(slot, 1 - core):
                cp.wait_recv()
            tb = tbuf[slot, 1]
            nbuf[0:TILE, :] = tb
            nbuf[TILE:512, :] = dot(dot(tbuf[slot, 0], gab[slot], 1, 0), tb, 1, 0)

        def gathered(h):
            return jnp.logical_and(h >= GATHER, h < last)

        def pairwise(h):
            return jnp.logical_or(h < GATHER, h == last)

        def product(h, slot, run):
            t0 = rows // TILE - tiles_of(h)

            def group(i, _):
                p = 1 - i
                wacc[p] = jnp.zeros((TILE, TILE), F32)
                lanes = pl.ds(pl.multiple_of(TILE * p, TILE), TILE)

                def one(t, n):
                    wacc[p] += dot6([(split(xt[t0 + t + u]), parts(slot, t + u, lanes)) for u in range(n)], 1, 0)
                run(tiles_of(h), one)
                if run is whole:
                    @pl.when(gathered(h))
                    def _():
                        for f in PAIR:
                            w_e1(p, f).start()

                    @pl.when(h < GATHER)
                    def _():
                        for half in PAIR:
                            w_p1(p, half).start()
                else:
                    for half in PAIR:
                        w_p1(p, half).start()
                return 0
            lax.fori_loop(0, 2, group, 0)

        def act_w(p):
            for half in PAIR:
                w_p1(p, half).wait()
            ws[p] = wacc[p] + r1[p]
            for half in PAIR:
                w_p2(p, half).start()

        def reduced(h, p):
            @pl.when(gathered(h))
            def _():
                for f in PAIR:
                    w_e3(p, f).wait()

            @pl.when(pairwise(h))
            def _():
                for half in PAIR:
                    w_p2(p, half).wait()
                wacc[p] = ws[p] + r2[p]
            return wacc[p]

        def update(h, slot, p, y):
            for k, part in enumerate(split(-y)):
                yp[k] = part
            t0 = rows // TILE - tiles_of(h)

            def one(t, n):
                for u in range(n):
                    xt[t0 + t + u] += dot6([(tuple(yp[k] for k in range(3)), parts(slot, t + u, pl.ds(TILE * p, TILE)))], 1, 1)
            whole(tiles_of(h), one)

        def ready(h, slot):
            collect_v(h)
            prepare(h, slot, 0, tiles_of(h))
            gram_own(h, slot)
            gram_cross(h, slot)

        top = rows // TILE - 1
        issue_v(last)
        v_loc(last).start()
        for part in PAIR:
            issue_z(top, part)
        for hh in range(last - 1, last - AHEAD, -1):
            issue_v(hh)
        v_loc(last - 1).start()
        for part in PAIR:
            issue_z(top - 1, part)
        clear_v()
        forward_v(last)
        ready(last, last % 3)
        send_g(last % 2, g_p1)
        collect_z(top)
        product(last, last % 3, lambda n, fn: fn(0, 1))
        forward_v(last - 1)
        v_loc(last - 2).start()
        ready(last - 1, (last - 1) % 3)
        act_p2(last % 2)
        act_w(1)
        act_w(0)
        send_g((last - 1) % 2, g_p1)
        forward_v(last - 2)

        def pick(k, n, fn):
            @pl.when(k >= 0)
            def _():
                lax.switch(k, [lambda hh=hh: fn(hh) for hh in range(n)])

        def block_step(i, _):
            h = last - i
            slot = h % 2
            vslot = h % 3

            @pl.when(jnp.logical_and(slot == 1, h < last))
            def _():
                collect_z((h - 1) // 2)

            @pl.when(h < last)
            def _():
                product(h, vslot, whole)

            @pl.when(pairwise(h))
            def _():
                merge(h, slot)

            @pl.when(h == last - 1)
            def _():
                act_p2(slot)

            @pl.when(jnp.logical_and(h > 1, h < GATHER))
            def _():
                act_rs2(1 - slot)
            pick(h - AHEAD, blocks - AHEAD, issue_v)

            nb = h - 2 + (blocks + 1 - h) // blocks
            active = jnp.logical_or(h > 2, h == 1)

            @pl.when(active)
            def _():
                pick(nb, blocks - 2, collect_v)

            n2 = tiles_of(nb)
            part = EARLY * n2 // 8
            cut = part + (n2 - part) * ((h + blocks - GATHER) // blocks)

            @pl.when(active)
            def _():
                prepare(nb, nb % 3, 0, cut)

            @pl.when(h < GATHER)
            def _():
                act_w(1)

            @pl.when(jnp.logical_and(active, h < GATHER))
            def _():
                prepare(nb, nb % 3, cut, n2)

            @pl.when(active)
            def _():
                gram_own(nb, nb % 3)

            @pl.when(gathered(h))
            def _():
                w_act1(1)

            @pl.when(h < GATHER)
            def _():
                act_w(0)

            @pl.when(active)
            def _():
                gram_cross(nb, nb % 3)
            pick(h - 3, blocks - 3, lambda hh: v_loc(hh).start())

            @pl.when(gathered(h))
            def _():
                w_act1(0)
                merge(h, slot)
                act_rs2(1 - slot)
                w_act2(1)
                w_act2(0)

            @pl.when(jnp.logical_and(h > 1, h < last))
            def _():
                act_ag2(1 - slot)

            @pl.when(h > 2)
            def _():
                send_g(slot)

            @pl.when(h == 1)
            def _():
                send_g(0, g_p1)

            @pl.when(jnp.logical_and(h < last, h >= last - top + 1))
            def _():
                for part in PAIR:
                    issue_z(h - (last - top + 1), part)

            @pl.when(jnp.logical_or(h > 3, h == 2))
            def _():
                pick(h - 3 + (blocks + 2 - h) // blocks, blocks - 3, forward_v)
            factor(slot)
            yb = dot(reduced(h, 1), nbuf[...], 1, 1)
            ws[1] = yb[:, TILE:512]
            update(h, vslot, 1, yb[:, 0:TILE])
            ya = dot(reduced(h, 0), tbuf[slot, 0], 1, 1) - ws[1]
            update(h, vslot, 0, ya)

            @pl.when(jnp.logical_and(h > 1, h < last))
            def _():
                act_ag1(1 - slot)

            @pl.when(h == 1)
            def _():
                act_p2(0)
            return 0

        lax.fori_loop(0, blocks, block_step, 0)
        out = pltpu.make_async_copy(xt, o_hbm, o_s)
        out.start()
        for hh in range(blocks):
            v_x(hh).wait_send()
            v_sib(hh).wait_send()
            v_fwd(hh).wait_send()
            for cp in t_copies(hh):
                cp.wait_send()
        for t in range(rows // TILE):
            for part in PAIR:
                for cp in z_copies(t, part):
                    cp.wait_send()
        out.wait()

    return body


def solution(mesh):
    def local(v_loc, t_loc, z_loc):
        rows, cols = v_loc.shape
        blocks = cols // LANE
        t_loc = t_loc.reshape(blocks, 2, WIDE, WIDE)
        tiles = ((blocks + 1) // 2) * ((blocks + 2) // 2)
        dma = pltpu.SemaphoreType.DMA
        hbm = pl.BlockSpec(memory_space=pl.ANY)
        xt = pl.pallas_call(
            make_kernel(rows, blocks),
            out_shape=jax.ShapeDtypeStruct((rows // TILE, TILE, TILE), F32),
            in_specs=[hbm] * 3,
            out_specs=hbm,
            scratch_shapes=[
                pltpu.VMEM((3 * TILE * tiles + 2 * rows, LANE), F32),
                pltpu.VMEM((3, 3, rows, 512), BF16),
                pltpu.VMEM((4, blocks, WIDE, WIDE), F32),
                pltpu.VMEM((rows // TILE, TILE, TILE), F32),
                pltpu.VMEM((2, TILE, TILE), F32), pltpu.VMEM((2, TILE, TILE), F32),
                pltpu.VMEM((2, TILE, TILE), F32), pltpu.VMEM((2, TILE, TILE), F32),
                pltpu.VMEM((3, TILE, TILE), BF16),
                pltpu.VMEM((384, TILE), F32),
                pltpu.VMEM((2, 448, LANE), F32), pltpu.VMEM((2, 448, LANE), F32),
                pltpu.VMEM((2, 448, LANE), F32), pltpu.VMEM((2, 448, LANE), F32),
                pltpu.VMEM((2, 2, TILE, TILE), F32),
                pltpu.VMEM((2, TILE, TILE), F32),
                pltpu.VMEM((512, TILE), F32),
                dma((blocks,)), dma((blocks,)), dma((blocks,)), dma((blocks,)), dma((3, blocks)),
                dma((blocks,)), dma((blocks,)), dma((blocks,)), dma((blocks,)), dma((4, blocks)),
                dma((3, rows // TILE, 2)), dma((rows // TILE, 2)), dma((4, rows // TILE, 2)),
                dma((2, 2)), dma((2, 2)), dma((2, 2)), dma((2, 2)),
                dma((4, 2, 2)), dma((4, 2, 2)), dma((4, 2, 2)), dma((4, 2, 2)),
                dma((2, 2)), dma((2, 2)), dma,
            ],
            compiler_params=pltpu.CompilerParams(collective_id=0, has_side_effects=True,
                                                 vmem_limit_bytes=67043328),
        )(v_loc, t_loc, z_loc.T)

        return xt.transpose(0, 2, 1).reshape(rows, TILE)

    return jax.shard_map(local, mesh=mesh,
                         in_specs=(P('row', 'col'), P('col', None, None), P(None, ('col', 'row'))),
                         out_specs=P('row', 'col'), check_vma=False)
```

```python
import jax
import jax.numpy as jnp
from jax import lax
from jax.experimental import pallas as pl
from jax.experimental.pallas import tpu as pltpu
from jax.sharding import PartitionSpec as P

F32 = jnp.float32
BF16 = jnp.bfloat16
MESH = pl.DeviceIdType.MESH
TILE = 256
LANE = 128
WIDE = 64
PAIR = range(2)
AHEAD = 8
GATHER = 8
EARLY = 4


def dot(a, b, ca, cb):
    return lax.dot_general(a, b, (((ca,), (cb,)), ((), ())), preferred_element_type=F32,
                           precision=lax.Precision.HIGHEST)


def split(a):
    a1 = a.astype(BF16)
    rest = a - a1.astype(F32)
    a2 = rest.astype(BF16)
    return a1, a2, (rest - a2.astype(F32)).astype(BF16)


def dot6(pairs, ca, cb):
    lhs, rhs = [], []
    for (a1, a2, a3), (b1, b2, b3) in pairs:
        lhs += [a3, a1, a2, a1, a2, a1]
        rhs += [b1, b3, b2, b2, b1, b1]
    return lax.dot_general(jnp.concatenate(lhs, ca), jnp.concatenate(rhs, cb), (((ca,), (cb,)), ((), ())),
                           preferred_element_type=F32)


def make_kernel(rows, blocks):
    def tiles_of(h):
        return (blocks + 1 - h) // 2

    def tiles_before(h):
        k = blocks - 1 - h
        return ((k + 1) // 2) * ((k + 2) // 2)

    area = TILE * tiles_before(-1)

    def body(v_hbm, t_hbm, z_hbm, o_hbm, vbuf, vp, tall, xt, wacc, r1, ws, r2, yp, gkk, gacc, gr1, gr2, gf, tbuf, gab,
             nbuf, vx_s, vsib_s, vfwd_s, vloc_s, v_r, tx_s, txc_s, tsib_s, tloc_s, t_r, z_s, zloc_s, z_r,
             p1_s, p1_r, p2_s, p2_r, g_s, g_r, w_s, w_r, d_s, d_r, o_s):
        r = lax.axis_index("row")
        c = lax.axis_index("col")
        core = c % 2
        cx, csib, cxc = (c + 2) % 4, c + 1 - 2 * core, 3 - c
        ry, rz, rd = r + 1 - 2 * (r % 2), (r + 2) % 4, 3 - r
        dev_x, dev_sib, dev_xc = (r, cx), (r, csib), (r, cxc)
        dev_y, dev_z, dev_d = (ry, c), (rz, c), (rd, c)

        last = blocks - 1

        def remote(src, dst, ss, rs, dev):
            return pltpu.make_async_remote_copy(src, dst, ss, rs, device_id=dev, device_id_type=MESH)

        barrier = pltpu.get_barrier_semaphore()
        for dev in (dev_x, dev_sib, dev_xc, dev_y, dev_z, dev_d):
            pl.semaphore_signal(barrier, 1, device_id=dev, device_id_type=MESH)
        pl.semaphore_wait(barrier, 6)

        def v_src(hh):
            n = LANE * (blocks - hh)
            return v_hbm.at[pl.ds(rows - n, n), pl.ds(hh * LANE, LANE)]

        def v_rows(base, hh):
            return vbuf.at[pl.ds(base + LANE * (hh % 2), LANE * (blocks - hh)), :]

        def v_dst(rel, hh):
            return v_rows(area * (rel - 1) + TILE * tiles_before(hh), hh)

        def v_x(hh):
            return remote(v_src(hh), v_dst(2, hh), vx_s.at[hh], v_r.at[1, hh], dev_x)

        def v_sib(hh):
            return remote(v_src(hh), v_dst(1, hh), vsib_s.at[hh], v_r.at[0, hh], dev_sib)

        def v_fwd(hh):
            return remote(v_dst(2, hh), v_dst(3, hh), vfwd_s.at[hh], v_r.at[2, hh], dev_sib)

        def v_loc(hh):
            return pltpu.make_async_copy(v_src(hh), v_rows(3 * area + rows * (hh % 2), hh), vloc_s.at[hh])

        def clear_v():
            for rel in range(3):
                for hh in range(1, blocks, 2):
                    vbuf[pl.ds(area * rel + TILE * tiles_before(hh), LANE), :] = jnp.zeros((LANE, LANE), F32)
            vbuf[pl.ds(3 * area + rows, LANE), :] = jnp.zeros((LANE, LANE), F32)

        def v_arrive(rel, hh):
            return remote(v_src(hh), v_dst(rel, hh), vx_s.at[hh], v_r.at[rel - 1, hh], dev_x)

        def t_copies(h):
            return (remote(t_hbm.at[h, core], tall.at[c, h], tx_s.at[h], t_r.at[c, h], dev_x),
                    remote(t_hbm.at[h, 1 - core], tall.at[c, h], txc_s.at[h], t_r.at[c, h], dev_xc),
                    remote(t_hbm.at[h, 1 - core], tall.at[c, h], tsib_s.at[h], t_r.at[c, h], dev_sib))

        def t_loc(h):
            return pltpu.make_async_copy(t_hbm.at[h, core], tall.at[c, h], tloc_s.at[h])

        def t_arrive(slot, h):
            return remote(t_hbm.at[h, core], tall.at[slot, h], tx_s.at[h], t_r.at[slot, h], dev_x)

        def issue_v(hh):
            v_x(hh).start()
            v_sib(hh).start()
            for cp in t_copies(hh):
                cp.start()
            t_loc(hh).start()

        def forward_v(hh):
            v_arrive(2, hh).wait_recv()
            v_fwd(hh).start()

        def collect_v(hh):
            v_loc(hh).wait()
            v_arrive(1, hh).wait_recv()
            v_arrive(3, hh).wait_recv()
            t_loc(hh).wait()
            for slot in (cx, csib, cxc):
                t_arrive(slot, hh).wait_recv()

        def z_src(to, t, part):
            return z_hbm.at[:, pl.ds(pl.multiple_of(rows * to + TILE * t + LANE * part, LANE), LANE)]

        def z_dst(src_r, t, part):
            return xt.at[t, pl.ds(pl.multiple_of(WIDE * src_r, WIDE), WIDE), pl.ds(LANE * part, LANE)]

        def z_copies(t, part):
            return [remote(z_src(dev[0], t, part), z_dst(r, t, part), z_s.at[i, t, part], z_r.at[r, t, part], dev)
                    for i, dev in enumerate((dev_y, dev_z, dev_d))]

        def z_loc(t, part):
            return pltpu.make_async_copy(z_src(r, t, part), z_dst(r, t, part), zloc_s.at[t, part])

        def issue_z(t, part):
            for cp in z_copies(t, part):
                cp.start()
            z_loc(t, part).start()

        def collect_z(t):
            for part in PAIR:
                z_loc(t, part).wait()
                for src_r in (ry, rz, rd):
                    dst = z_dst(src_r, t, part)
                    remote(z_src(r, t, part), dst, z_s.at[0, t, part], z_r.at[src_r, t, part], dev_y).wait_recv()

        def steps(half):
            return (dev_y, dev_z) if half == 0 else (dev_z, dev_y)

        def w_p1(p, half):
            s = pl.ds(LANE * half, LANE)
            return remote(wacc.at[p, s], r1.at[p, s], p1_s.at[p, half], p1_r.at[p, half], steps(half)[0])

        def w_p2(p, half):
            s = pl.ds(LANE * half, LANE)
            return remote(ws.at[p, s], r2.at[p, s], p2_s.at[p, half], p2_r.at[p, half], steps(half)[1])

        def g_place(f):
            k1, k2 = ((r % 2), (r // 2)) if f == 0 else ((r // 2), (r % 2))
            return 224 * f, k1, k2

        def g_rows(start, n):
            return pl.ds(pl.multiple_of(start, 8), n)

        def w_kept(f, other=0):
            k1 = r % 2 if f == 0 else r // 2
            return g_rows(LANE * f + WIDE * (k1 + other * (1 - 2 * k1)), WIDE)

        def w_e1(p, f):
            s = w_kept(f, 1)
            return remote(wacc.at[p, s], r1.at[p, s], w_s.at[0, p, f], w_r.at[0, p, f], steps(f)[0])

        def w_e2(p, f):
            s = w_kept(f)
            return remote(ws.at[p, s], r2.at[p, s], w_s.at[1, p, f], w_r.at[1, p, f], steps(f)[1])

        def w_e3(p, f):
            s = w_kept(f)
            return remote(wacc.at[p, s], wacc.at[p, s], w_s.at[2, p, f], w_r.at[2, p, f], steps(f)[0])

        def w_act1(p):
            for f in PAIR:
                w_e1(p, f).wait()
            for f in PAIR:
                s = w_kept(f)
                ws[p, s] = wacc[p, s] + r1[p, s]
                w_e2(p, f).start()

        def w_act2(p):
            for f in PAIR:
                w_e2(p, f).wait()
            for f in PAIR:
                s = w_kept(f)
                wacc[p, s] = ws[p, s] + r2[p, s]
                w_e3(p, f).start()

        def g_p1(par, f):
            s = pl.ds(224 * f, 224)
            return remote(gacc.at[par, s], gr1.at[par, s], g_s.at[0, par, f], g_r.at[0, par, f], steps(f)[0])

        def g_p2(par, f):
            s = pl.ds(224 * f, 224)
            return remote(gacc.at[par, s], gr2.at[par, s], g_s.at[1, par, f], g_r.at[1, par, f], steps(f)[1])

        def act_p2(par):
            for f in PAIR:
                g_p1(par, f).wait()
            gacc[par] = gacc[par] + gr1[par]
            for f in PAIR:
                g_p2(par, f).start()

        def g_rs1(par, f):
            base, k1, _ = g_place(f)
            s = g_rows(base + 112 * (1 - k1), 112)
            return remote(gacc.at[par, s], gr1.at[par, s], g_s.at[0, par, f], g_r.at[0, par, f], steps(f)[0])

        def g_rs2(par, f):
            base, k1, k2 = g_place(f)
            s = g_rows(base + 112 * k1 + 56 * (1 - k2), 56)
            return remote(gacc.at[par, s], gr2.at[par, s], g_s.at[1, par, f], g_r.at[1, par, f], steps(f)[1])

        def g_ag2(par, f):
            base, k1, k2 = g_place(f)
            s = g_rows(base + 112 * k1 + 56 * k2, 56)
            return remote(gf.at[par, s], gf.at[par, s], g_s.at[2, par, f], g_r.at[2, par, f], steps(f)[1])

        def g_ag1(par, f):
            base, k1, _ = g_place(f)
            s = g_rows(base + 112 * k1, 112)
            return remote(gf.at[par, s], gf.at[par, s], g_s.at[3, par, f], g_r.at[3, par, f], steps(f)[0])

        def act_rs2(par):
            for f in PAIR:
                g_rs1(par, f).wait()
            for f in PAIR:
                base, k1, _ = g_place(f)
                s = g_rows(base + 112 * k1, 112)
                gacc[par, s] = gacc[par, s] + gr1[par, s]
                g_rs2(par, f).start()

        def act_ag2(par):
            for f in PAIR:
                base, k1, k2 = g_place(f)
                g_rs2(par, f).wait()
                s = g_rows(base + 112 * k1 + 56 * k2, 56)
                gf[par, s] = gacc[par, s] + gr2[par, s]
                g_ag2(par, f).start()

        def act_ag1(par):
            for f in PAIR:
                g_ag2(par, f).wait()
                g_ag1(par, f).start()

        def over_tiles(n, fn):
            def four(t, _):
                fn(4 * t, 4)
                return 0
            lax.fori_loop(0, n // 4, four, 0)

            @pl.when(n % 4 >= 2)
            def _():
                fn(4 * (n // 4), 2)

            @pl.when(n % 2 == 1)
            def _():
                fn(n - 1, 1)

        def whole(n, fn):
            for k in range(1, rows // TILE + 1):
                @pl.when(n == k)
                def _():
                    fn(0, k)

        def prepare(h, slot, start, stop):
            bases = []
            for i in range(4):
                rel = ((c // 2 + i // 2) % 2) * 2 + (c + i) % 2
                own = (3 - rel) // 3
                bases.append(own * (3 * area + rows * (h % 2)) + (1 - own) * (area * (rel - 1) + TILE * tiles_before(h)))

            def one(t, _):
                d = pl.ds(pl.multiple_of(TILE * t, TILE), TILE)
                for i in PAIR:
                    a = vbuf[pl.ds(pl.multiple_of(bases[2 * i] + TILE * t, TILE), TILE), :]
                    b = vbuf[pl.ds(pl.multiple_of(bases[2 * i + 1] + TILE * t, TILE), TILE), :]
                    low = lax.broadcasted_iota(jnp.int32, a.shape, 1) < WIDE
                    ar, br = pltpu.roll(a, WIDE, 1), pltpu.roll(b, WIDE, 1)
                    for k, part in enumerate(split(jnp.where(low, a, br))):
                        vp[slot, k, d, LANE * i:LANE * i + LANE] = part
                    for k, part in enumerate(split(jnp.where(low, ar, b))):
                        vp[slot, k, d, TILE + LANE * i:TILE + LANE * i + LANE] = part
                return 0
            lax.fori_loop(start, stop, one, 0)

        def parts(slot, t, lanes):
            s = pl.ds(pl.multiple_of(TILE * t, TILE), TILE)
            return tuple(vp[slot, k, s, lanes] for k in range(3))

        top3 = LANE + WIDE

        def gram_own(h, slot):
            gkk[0:top3, :] = jnp.zeros((top3, TILE), F32)
            mine = pl.ds(pl.multiple_of(TILE * core, TILE), TILE)

            def one(t, n):
                own = [parts(slot, t + u, mine) for u in range(n)]
                gkk[0:top3, :] += dot6([(tuple(x[:, 0:top3] for x in a), a) for a in own], 0, 0)
            over_tiles(tiles_of(h), one)

        def gram_cross(h, slot):
            gkk[TILE:TILE + LANE, :] = jnp.zeros((LANE, TILE), F32)
            half = pl.ds(pl.multiple_of(LANE * core, LANE), LANE)

            def one(t, n):
                gkk[TILE:TILE + LANE, :] += dot6([(parts(slot, t + u, half), parts(slot, t + u, pl.ds(TILE, TILE)))
                                                  for u in range(n)], 0, 0)
            over_tiles(tiles_of(h), one)

        def send_g(par, first=g_rs1):
            gacc[par, 0:LANE, :] = gkk[TILE:384, 0:LANE]
            gacc[par, LANE:TILE, :] = gkk[TILE:384, LANE:TILE]
            gacc[par, TILE:384, :] = gkk[0:LANE, LANE:TILE]
            gacc[par, 384:448, 0:WIDE] = gkk[0:WIDE, WIDE:LANE]
            gacc[par, 384:448, WIDE:LANE] = gkk[LANE:192, 192:TILE]
            for f in PAIR:
                first(par, f).start()

        def rows_of(k):
            return pl.ds(pl.multiple_of(LANE * k, LANE), LANE)

        def share(slot, k):
            return (remote(tbuf.at[slot, k], tbuf.at[slot, k], d_s.at[slot, 0], d_r.at[slot, 0], dev_sib),
                    remote(gab.at[slot, rows_of(k)], gab.at[slot, rows_of(k)], d_s.at[slot, 1], d_r.at[slot, 1], dev_sib))

        def merge(h, slot):
            @pl.when(jnp.logical_or(h >= last - 1, h == 0))
            def _():
                for f in PAIR:
                    g_p2(slot, f).wait()
                gf[slot] = gacc[slot] + gr2[slot]

            @pl.when(jnp.logical_and(h > 0, h < last - 1))
            def _():
                for f in PAIR:
                    g_ag1(slot, f).wait()
            g = gf[slot]
            gab[slot, rows_of(core), 0:LANE] = g[0:LANE]
            gab[slot, rows_of(core), LANE:TILE] = g[LANE:TILE]
            zero = jnp.zeros((WIDE, WIDE), F32)

            def diag(a, b):
                return jnp.concatenate([jnp.concatenate([a, zero], 1), jnp.concatenate([zero, b], 1)], 0)
            t0, t1, t2, t3 = (tall[i, h] for i in range(4))
            low = g[384:448]
            off = dot(diag(low[:, 0:WIDE], low[:, WIDE:LANE]), diag(t1, t3), 1, 0)
            off = -dot(diag(t0, t2), off, 1, 0)
            ta = jnp.concatenate([jnp.concatenate([t0, off[0:WIDE, 0:WIDE]], 1), jnp.concatenate([zero, t1], 1)], 0)
            tb = jnp.concatenate([jnp.concatenate([t2, off[WIDE:LANE, WIDE:LANE]], 1), jnp.concatenate([zero, t3], 1)], 0)
            cross = -dot(ta, dot(g[TILE:384], tb, 1, 0), 1, 0)
            tbuf[slot, core, 0:LANE, 0:LANE] = ta
            tbuf[slot, core, 0:LANE, LANE:TILE] = cross
            tbuf[slot, core, LANE:TILE, 0:LANE] = jnp.zeros((LANE, LANE), F32)
            tbuf[slot, core, LANE:TILE, LANE:TILE] = tb
            for cp in share(slot, core):
                cp.start()

        def factor(slot):
            for cp in share(slot, core):
                cp.wait_send()
            for cp in share(slot, 1 - core):
                cp.wait_recv()
            tb = tbuf[slot, 1]
            nbuf[0:TILE, :] = tb
            nbuf[TILE:512, :] = dot(dot(tbuf[slot, 0], gab[slot], 1, 0), tb, 1, 0)

        def gathered(h):
            return jnp.logical_and(h >= GATHER, h < last)

        def pairwise(h):
            return jnp.logical_or(h < GATHER, h == last)

        def product(h, slot, run):
            t0 = rows // TILE - tiles_of(h)

            def group(i, _):
                p = 1 - i
                wacc[p] = jnp.zeros((TILE, TILE), F32)
                lanes = pl.ds(pl.multiple_of(TILE * p, TILE), TILE)

                def one(t, n):
                    wacc[p] += dot6([(split(xt[t0 + t + u]), parts(slot, t + u, lanes)) for u in range(n)], 1, 0)
                run(tiles_of(h), one)
                if run is whole:
                    @pl.when(gathered(h))
                    def _():
                        for f in PAIR:
                            w_e1(p, f).start()

                    @pl.when(h < GATHER)
                    def _():
                        for half in PAIR:
                            w_p1(p, half).start()
                else:
                    for half in PAIR:
                        w_p1(p, half).start()
                return 0
            lax.fori_loop(0, 2, group, 0)

        def act_w(p):
            for half in PAIR:
                w_p1(p, half).wait()
            ws[p] = wacc[p] + r1[p]
            for half in PAIR:
                w_p2(p, half).start()

        def reduced(h, p):
            @pl.when(gathered(h))
            def _():
                for f in PAIR:
                    w_e3(p, f).wait()

            @pl.when(pairwise(h))
            def _():
                for half in PAIR:
                    w_p2(p, half).wait()
                wacc[p] = ws[p] + r2[p]
            return wacc[p]

        def update(h, slot, p, y):
            for k, part in enumerate(split(-y)):
                yp[k] = part
            t0 = rows // TILE - tiles_of(h)

            def one(t, n):
                for u in range(n):
                    xt[t0 + t + u] += dot6([(tuple(yp[k] for k in range(3)), parts(slot, t + u, pl.ds(TILE * p, TILE)))], 1, 1)
            whole(tiles_of(h), one)

        def ready(h, slot):
            collect_v(h)
            prepare(h, slot, 0, tiles_of(h))
            gram_own(h, slot)
            gram_cross(h, slot)

        top = rows // TILE - 1
        issue_v(last)
        v_loc(last).start()
        for part in PAIR:
            issue_z(top, part)
        for hh in range(last - 1, last - AHEAD, -1):
            issue_v(hh)
        v_loc(last - 1).start()
        for part in PAIR:
            issue_z(top - 1, part)
        clear_v()
        forward_v(last)
        ready(last, last % 3)
        send_g(last % 2, g_p1)
        collect_z(top)
        product(last, last % 3, lambda n, fn: fn(0, 1))
        forward_v(last - 1)
        v_loc(last - 2).start()
        ready(last - 1, (last - 1) % 3)
        act_p2(last % 2)
        act_w(1)
        act_w(0)
        send_g((last - 1) % 2, g_p1)
        forward_v(last - 2)

        def pick(k, n, fn):
            @pl.when(k >= 0)
            def _():
                lax.switch(k, [lambda hh=hh: fn(hh) for hh in range(n)])

        def block_step(i, _):
            h = last - i
            slot = h % 2
            vslot = h % 3

            @pl.when(jnp.logical_and(slot == 1, h < last))
            def _():
                collect_z((h - 1) // 2)

            @pl.when(h < last)
            def _():
                product(h, vslot, whole)

            @pl.when(jnp.logical_and(pairwise(h), h > 0))
            def _():
                merge(h, slot)

            @pl.when(h == last - 1)
            def _():
                act_p2(slot)

            @pl.when(jnp.logical_and(h > 1, h < GATHER))
            def _():
                act_rs2(1 - slot)
            pick(h - AHEAD, blocks - AHEAD, issue_v)

            nb = h - 2 + (blocks + 1 - h) // blocks
            active = jnp.logical_or(h > 2, h == 1)

            @pl.when(active)
            def _():
                pick(nb, blocks - 2, collect_v)

            n2 = tiles_of(nb)
            part = EARLY * n2 // 8
            cut = part + (n2 - part) * ((h + blocks - GATHER) // blocks)

            @pl.when(active)
            def _():
                prepare(nb, nb % 3, 0, cut)

            @pl.when(h < GATHER)
            def _():
                act_w(1)

            @pl.when(h == 0)
            def _():
                merge(h, slot)

            @pl.when(jnp.logical_and(active, h < GATHER))
            def _():
                prepare(nb, nb % 3, cut, n2)

            @pl.when(active)
            def _():
                gram_own(nb, nb % 3)

            @pl.when(gathered(h))
            def _():
                w_act1(1)

            @pl.when(h < GATHER)
            def _():
                act_w(0)

            @pl.when(active)
            def _():
                gram_cross(nb, nb % 3)
            pick(h - 3, blocks - 3, lambda hh: v_loc(hh).start())

            @pl.when(gathered(h))
            def _():
                w_act1(0)
                merge(h, slot)
                act_rs2(1 - slot)
                w_act2(1)
                w_act2(0)

            @pl.when(jnp.logical_and(h > 1, h < last))
            def _():
                act_ag2(1 - slot)

            @pl.when(h > 2)
            def _():
                send_g(slot)

            @pl.when(h == 1)
            def _():
                send_g(0, g_p1)

            @pl.when(jnp.logical_and(h < last, h >= last - top + 1))
            def _():
                for part in PAIR:
                    issue_z(h - (last - top + 1), part)

            @pl.when(jnp.logical_or(h > 3, h == 2))
            def _():
                pick(h - 3 + (blocks + 2 - h) // blocks, blocks - 3, forward_v)
            factor(slot)
            yb = dot(reduced(h, 1), nbuf[...], 1, 1)
            ws[1] = yb[:, TILE:512]
            update(h, vslot, 1, yb[:, 0:TILE])
            ya = dot(reduced(h, 0), tbuf[slot, 0], 1, 1) - ws[1]
            update(h, vslot, 0, ya)

            @pl.when(jnp.logical_and(h > 1, h < last))
            def _():
                act_ag1(1 - slot)

            @pl.when(h == 1)
            def _():
                act_p2(0)
            return 0

        lax.fori_loop(0, blocks, block_step, 0)
        out = pltpu.make_async_copy(xt, o_hbm, o_s)
        out.start()
        for hh in range(blocks):
            v_x(hh).wait_send()
            v_sib(hh).wait_send()
            v_fwd(hh).wait_send()
            for cp in t_copies(hh):
                cp.wait_send()
        for t in range(rows // TILE):
            for part in PAIR:
                for cp in z_copies(t, part):
                    cp.wait_send()
        out.wait()

    return body


def solution(mesh):
    def local(v_loc, t_loc, z_loc):
        rows, cols = v_loc.shape
        blocks = cols // LANE
        t_loc = t_loc.reshape(blocks, 2, WIDE, WIDE)
        tiles = ((blocks + 1) // 2) * ((blocks + 2) // 2)
        dma = pltpu.SemaphoreType.DMA
        hbm = pl.BlockSpec(memory_space=pl.ANY)
        xt = pl.pallas_call(
            make_kernel(rows, blocks),
            out_shape=jax.ShapeDtypeStruct((rows // TILE, TILE, TILE), F32),
            in_specs=[hbm] * 3,
            out_specs=hbm,
            scratch_shapes=[
                pltpu.VMEM((3 * TILE * tiles + 2 * rows, LANE), F32),
                pltpu.VMEM((3, 3, rows, 512), BF16),
                pltpu.VMEM((4, blocks, WIDE, WIDE), F32),
                pltpu.VMEM((rows // TILE, TILE, TILE), F32),
                pltpu.VMEM((2, TILE, TILE), F32), pltpu.VMEM((2, TILE, TILE), F32),
                pltpu.VMEM((2, TILE, TILE), F32), pltpu.VMEM((2, TILE, TILE), F32),
                pltpu.VMEM((3, TILE, TILE), BF16),
                pltpu.VMEM((384, TILE), F32),
                pltpu.VMEM((2, 448, LANE), F32), pltpu.VMEM((2, 448, LANE), F32),
                pltpu.VMEM((2, 448, LANE), F32), pltpu.VMEM((2, 448, LANE), F32),
                pltpu.VMEM((2, 2, TILE, TILE), F32),
                pltpu.VMEM((2, TILE, TILE), F32),
                pltpu.VMEM((512, TILE), F32),
                dma((blocks,)), dma((blocks,)), dma((blocks,)), dma((blocks,)), dma((3, blocks)),
                dma((blocks,)), dma((blocks,)), dma((blocks,)), dma((blocks,)), dma((4, blocks)),
                dma((3, rows // TILE, 2)), dma((rows // TILE, 2)), dma((4, rows // TILE, 2)),
                dma((2, 2)), dma((2, 2)), dma((2, 2)), dma((2, 2)),
                dma((4, 2, 2)), dma((4, 2, 2)), dma((4, 2, 2)), dma((4, 2, 2)),
                dma((2, 2)), dma((2, 2)), dma,
            ],
            compiler_params=pltpu.CompilerParams(collective_id=0, has_side_effects=True,
                                                 vmem_limit_bytes=67043328),
        )(v_loc, t_loc, z_loc.T)

        return xt.transpose(0, 2, 1).reshape(rows, TILE)

    return jax.shard_map(local, mesh=mesh,
                         in_specs=(P('row', 'col'), P('col', None, None), P(None, ('col', 'row'))),
                         out_specs=P('row', 'col'), check_vma=False)
```
